128 devices in a mesh: gx: 8 (over z, core), gy: 16 (over x, y).
Axes of the slice: x: 4, y: 4, z: 4, core: 2. Of those that a mesh axis runs over, the one named last changes fastest.
Arguments:
- table: float32 [1048576, 128], P(('gx', 'gy')), may hold values from -6 to 6
- accum: float32 [1048576], P(('gx', 'gy')), may hold values from 0.05 to 1
- cache_values: float32 [524288, 128], P(('gx', 'gy')), may hold values from -6 to 6
- cache_rows: int32 [524288], P(('gx', 'gy')), may hold values from 0 to 1048575, as said below
- pending: float32 [524288, 128], P(('gx', 'gy')), may hold values from -3 to 3
- batch_slots: int32 [3, 65536, 16], P(None, ('gx', 'gy')), may hold values from 0 to 4095
- targets: float32 [3, 65536, 128], P(None, ('gx', 'gy')), may hold values from -6 to 6
- dirty: int32 [3, 65536], P(None, ('gx', 'gy')), may hold values from 0 to 4095, as said below
Outputs:
- new_table: float32 [1048576, 128], P(('gx', 'gy'))
- new_accum: float32 [1048576], P(('gx', 'gy'))
- new_cache: float32 [524288, 128], P(('gx', 'gy'))
- new_pending: float32 [524288, 128], P(('gx', 'gy'))
The draws below stay inside these ranges and needn't reach their ends.
Inputs may be any that keep to these rules, and one draw needn't show every extreme that they name: `cache_rows`: each device's slots form 128 blocks of 32 consecutive slots; every block holds rows of one owner, and every owner has exactly one block on every device. `dirty`: in each step a device's 512 entries are distinct slots of that device; at most 8 of them hold rows of one owner, and in every step some owner gets exactly 8 from every device.
All inputs are finite; a program needn't handle non-finite values.
Results may differ from the reference program's by a relative error of at most 0.0001.
Values sent between devices are 32-bit elements; how exact they have to be, the bound alone decides.
A program may use at most 128 MiB of HBM per device.

```python
import math
import jax
import jax.numpy as jnp
from jax import lax

W = 128
ROWS_DEV = 8192
CACHE = 4096
B_DEV = 512
BAG = 16
DIRTY = 512
STEPS = 3
DEVICES = 128


def owner_places(key):
    keys = jax.random.split(jax.random.fold_in(key, 101), DEVICES)
    return jax.vmap(lambda single: jax.random.permutation(single, DEVICES))(keys)


def draw_cache_rows(key, part):
    places = owner_places(key)
    per_block = CACHE // DEVICES
    block_owner = jnp.argsort(places, axis=1).astype(jnp.int32)
    local = jax.random.randint(jax.random.fold_in(key, 202), (DEVICES, DEVICES, per_block), 0, ROWS_DEV)
    holders = block_owner[:, :, None] * ROWS_DEV + local
    return holders.reshape(-1).astype(jnp.int32)


def dirty_step(key, places, step):
    per_block = CACHE // DEVICES
    capacity = 2 * DIRTY // DEVICES
    half = capacity // 2
    step_key = jax.random.fold_in(key, 300 + step)
    pairing = jax.random.permutation(jax.random.fold_in(step_key, 1), DEVICES)
    moves = jax.random.randint(jax.random.fold_in(step_key, 2), (DEVICES, DEVICES // 2), half // 2, half + 1)
    moves = moves.at[:, 0].set(half)
    counts = jnp.full((DEVICES, DEVICES), half, jnp.int32)
    counts = counts.at[:, pairing[0::2]].add(moves)
    counts = counts.at[:, pairing[1::2]].add(-moves)
    offsets = jax.random.randint(jax.random.fold_in(step_key, 3), (DEVICES, DEVICES), 0, per_block)
    within = jnp.arange(per_block, dtype=jnp.int32)
    chosen = within[None, None, :] < counts[:, :, None]
    slots = places[:, :, None] * per_block + (within[None, None, :] + offsets[:, :, None]) % per_block
    shuffle_keys = jax.random.split(jax.random.fold_in(step_key, 4), DEVICES)
    shuffles = jax.vmap(lambda single: jax.random.permutation(single, DEVICES * per_block))(shuffle_keys)
    scores = jnp.where(chosen.reshape(DEVICES, -1), 0, DEVICES * per_block) + shuffles
    order = jnp.argsort(scores, axis=1)[:, :DIRTY]
    return jnp.take_along_axis(slots.reshape(DEVICES, -1), order, axis=1)


def draw_dirty(key, part):
    places = owner_places(key)
    listed = jnp.stack([dirty_step(key, places, step) for step in range(STEPS)])
    return listed.reshape(STEPS, DEVICES * DIRTY).astype(jnp.int32)


def set_ends(values, stream_key, smallest, top_value):
    longest = values.shape.index(max(values.shape))
    spots = []
    for shift in (0, 1):
        where = [jax.random.randint(jax.random.fold_in(stream_key, axis), (), 0, length) for axis, length in enumerate(values.shape)]
        where[longest] = (where[longest] + shift) % values.shape[longest]
        spots.append(tuple(where))
    return values.at[spots[0]].set(smallest).at[spots[1]].set(top_value)


def steps_of(stream_key, shape, cuts, smallest, top_value):
    level = 1.0
    for position, shards_of in cuts:
        heights = jax.random.uniform(jax.random.fold_in(jax.random.fold_in(stream_key, 6), position), (shards_of,), jnp.float32, smallest / len(cuts), top_value / len(cuts))
        level = level * jnp.repeat(jnp.exp(heights), shape[position] // shards_of).reshape((-1,) + (1,) * (len(shape) - 1 - position))
    return level


def scatter_about(own_key, extent, deviation, most, cuts=(), kind=jnp.bfloat16):
    array = deviation * jax.random.normal(own_key, extent, jnp.float32)
    if cuts:
        array = array * steps_of(own_key, extent, cuts, -0.22, 0.18)
    return jnp.clip(array, -most, most).astype(kind)


def setup_inputs(seed: int = 0) -> dict:
    key_list = jax.random.split(jax.random.key(seed), 9)
    return {
        "table": scatter_about(key_list[0], (ROWS_DEV * DEVICES, W), 1.0, 6.0, ((0, 128),), jnp.float32),
        "accum": jnp.clip(jnp.exp(math.log(1.0) - 2.9957323 * jax.random.uniform(key_list[1], (ROWS_DEV * DEVICES,), jnp.float32) ** steps_of(key_list[1], (ROWS_DEV * DEVICES,), ((0, 128),), -0.2, 0.2)), 0.05, 1.0),
        "cache_values": scatter_about(key_list[2], (CACHE * DEVICES, W), 1.0, 6.0, ((0, 128),), jnp.float32),
        "cache_rows": draw_cache_rows(jax.random.fold_in(key_list[8], 71), 0),
        "pending": scatter_about(key_list[4], (CACHE * DEVICES, W), 0.3, 3.0, ((0, 128),), jnp.float32),
        "batch_slots": set_ends(jax.random.randint(key_list[5], (STEPS, B_DEV * DEVICES, BAG), 0, CACHE), jax.random.fold_in(key_list[5], 1), 0, CACHE - 1).astype(jnp.int32),
        "targets": scatter_about(key_list[6], (STEPS, B_DEV * DEVICES, W), 1.0, 6.0, ((1, 128),), jnp.float32),
        "dirty": draw_dirty(jax.random.fold_in(key_list[8], 71), 0),
    }


LEARN_RATE = 0.3

def local_grad(values, ids, goal):
    pooled = lax.optimization_barrier(jnp.mean(jnp.take(values, ids, axis=0), axis=1))
    bag_grad = (pooled - goal) / BAG
    spread = jnp.broadcast_to(bag_grad[:, None, :], (B_DEV, BAG, W)).reshape(-1, W)
    return jax.ops.segment_sum(spread, ids.reshape(-1), num_segments=CACHE)

def reference(table, accum, cache_values, cache_rows, pending, batch_slots, targets, dirty):
    cached = cache_values.reshape(DEVICES, CACHE, W)
    waiting = pending.reshape(DEVICES, CACHE, W)
    holders = cache_rows.reshape(DEVICES, CACHE)
    for step in range(STEPS):
        picks = batch_slots[step].reshape(DEVICES, B_DEV, BAG)
        wanted = targets[step].reshape(DEVICES, B_DEV, W)
        grads = lax.map(lambda item: local_grad(item[0], item[1], item[2]), (cached, picks, wanted))
        waiting = waiting + grads
        listed = dirty[step].reshape(DEVICES, DIRTY)
        flushed = jnp.take_along_axis(waiting, listed[:, :, None], axis=1)
        chosen_rows = jnp.take_along_axis(holders, listed, axis=1)
        table_grad = jnp.zeros_like(table).at[chosen_rows.reshape(-1)].add(flushed.reshape(-1, W))
        waiting = jax.vmap(lambda block, where: block.at[where].set(0.0))(waiting, listed)
        accum = accum + lax.optimization_barrier(jnp.mean(table_grad * table_grad, axis=1))
        table = table - LEARN_RATE * table_grad / jnp.sqrt(accum)[:, None]
        fresh = jnp.take(table, chosen_rows.reshape(-1), axis=0).reshape(DEVICES, DIRTY, W)
        cached = jax.vmap(lambda block, where, value: block.at[where].set(value))(cached, listed, fresh)
    return (table, accum, cached.reshape(-1, W), waiting.reshape(-1, W))
```

```python
import functools

import jax
import jax.numpy as jnp
from jax import lax
from jax.experimental import pallas as pl
from jax.experimental.pallas import tpu as pltpu
from jax.sharding import PartitionSpec as P

LEARN_RATE = 0.3
MESH = pl.DeviceIdType.MESH
F32, BF16, I32 = jnp.float32, jnp.bfloat16, jnp.int32

N = 128
CAP = 8
W = 128
SLOTS = 4096
BLOCK = 32
ROWS = 8192
BAGS = 512
BAG = 16
STEPS = 3
GROUPS = 4


def iota(shape, dim):
    return lax.broadcasted_iota(I32, shape, dim)


def one_hot(mask):
    return jnp.where(mask, 1.0, 0.0).astype(BF16)


def parts(x):
    hi = x.astype(BF16)
    return jnp.concatenate([hi, (x - hi.astype(F32)).astype(BF16)], axis=1)


def joined(y):
    return y[:, :W] + y[:, W:]


def dot(a, b):
    return jnp.dot(a, b, preferred_element_type=F32)


def dot_nt(a, b):
    return lax.dot_general(a, b, (((1,), (1,)), ((), ())), preferred_element_type=F32)


def dot_tn(a, b):
    return lax.dot_general(a, b, (((0,), (0,)), ((), ())), preferred_element_type=F32)


def exact_bf16(x):
    return x.astype(BF16)


def kernel(
    owner_sm, keys_ref, dirty_ref, rows_ref, accum_ref, table_hbm, cache_hbm, pending_hbm, targets_hbm,
    table_out, accum_out, cache_out, pending_out,
    table, cache, waiting, targets, counts, sel, mix, pick, base, flush, fresh, freshp, bag_grad,
    send_f, recv_f, send_b, recv_b, idx_send, idx_recv, idx_sm, inv_v, inv_sm,
    place, ycol, yrow, same, share, old, acc_old, delta,
    in_sem, sm_sem, out_sem, isend_sem, irecv_sem, fsend_sem, frecv_sem, bsend_sem, brecv_sem,
):
    gx, gy = lax.axis_index("gx"), lax.axis_index("gy")
    me = gx * 16 + gy

    def partner(k):
        p = lax.rem(me + k, N)
        return p, (p // 16, lax.rem(p, 16))

    loads = [
        pltpu.make_async_copy(cache_hbm, cache, in_sem.at[0]),
        pltpu.make_async_copy(targets_hbm, targets, in_sem.at[1]),
        pltpu.make_async_copy(pending_hbm, waiting, in_sem.at[2]),
        pltpu.make_async_copy(table_hbm, table, in_sem.at[3]),
    ]
    for load in loads:
        load.start()
    barrier = pltpu.get_barrier_semaphore()

    def greet(k, _):
        pl.semaphore_signal(barrier, inc=1, device_id=partner(k)[1], device_id_type=MESH)
        return 0

    lax.fori_loop(1, N, greet, 0)

    lane_i = iota((BLOCK, 256), 1)
    sub_i = iota((BLOCK, 256), 0)
    before = one_hot(sub_i < lane_i % BLOCK)
    spread = one_hot(sub_i == lane_i % BLOCK)
    rows = rows_ref[...]
    local = rows - (rows // ROWS) * ROWS
    local_hi = local // 128
    local_lo = local - local_hi * 128
    rep_hi = dot(exact_bf16(local_hi.astype(F32)), spread)
    rep_lo = dot(exact_bf16(local_lo.astype(F32)), spread)
    want = (iota((N, 256), 1) // BLOCK).astype(F32)
    inner = (iota((N, 256), 1) % BLOCK).astype(F32)
    found = jnp.zeros((N, W), F32)
    at_hi = jnp.zeros((N, W), F32)
    at_lo = jnp.zeros((N, W), F32)
    at_in = jnp.zeros((N, W), F32)
    for t in range(STEPS):
        d = dirty_ref[t : t + 1, :]
        blk = d // BLOCK
        hot_b = one_hot(iota((N, BAGS), 0) == blk)
        hot_i = one_hot(iota((BLOCK, BAGS), 0) == d - blk * BLOCK)
        listed = exact_bf16(dot_nt(hot_b, hot_i))
        rank = dot(listed, before)
        there = dot(listed, spread)
        chosen = jnp.where((rank == want) & (there > 0.5), 1.0, 0.0)
        gather = one_hot(iota((256, W), 0) // BLOCK + t * CAP == iota((256, W), 1))
        found = found + dot(exact_bf16(chosen), gather)
        at_hi = at_hi + dot(exact_bf16(chosen * rep_hi), gather)
        at_lo = at_lo + dot(exact_bf16(chosen * rep_lo), gather)
        at_in = at_in + dot(exact_bf16(chosen * inner), gather)
    owner_col = rows[:, :1] // ROWS
    perm = one_hot(owner_col == iota((N, N), 1))
    sent_found = dot_tn(perm, exact_bf16(found))
    sent_hi = dot_tn(perm, exact_bf16(at_hi))
    sent_lo = dot_tn(perm, exact_bf16(at_lo))
    sent = jnp.where(sent_found > 0.5, sent_hi * 128.0 + sent_lo, -1.0).astype(I32)
    idx_send[...] = sent.reshape(N, 1, W)
    block_row = exact_bf16(iota((8, N), 1).astype(F32))
    inv_v[...] = jnp.minimum(dot(block_row, perm), N - 1.0).astype(I32)
    inv_copy = pltpu.make_async_copy(inv_v, inv_sm, sm_sem.at[0])
    inv_copy.start()
    in_block = jnp.where(found > 0.5, at_in, -1.0)
    for t in range(STEPS):
        rep8 = one_hot(iota((W, 256), 0) == iota((W, 256), 1) % CAP + t * CAP)
        wide_in = dot(exact_bf16(in_block), rep8)
        for g in range(GROUPS):
            jj = iota((N, 256), 0) - g * 32
            here = jj == iota((N, 256), 1) // CAP
            part = exact_bf16(jnp.where(here, wide_in, 0.0))
            inside = dot(jnp.ones((8, N), BF16), part)
            offset = (iota((8, 256), 1) // CAP * BLOCK).astype(F32)
            place[t, g] = jnp.where(inside < -0.5, -1.0, inside + offset).astype(I32)

    def build_counts(t):
        def group(g, _):
            slot = keys_ref[t, pl.ds(g, 1), :]
            head = slot // 128
            key = head * 16 + iota((1, 256), 1) // BAG
            a = one_hot(iota((512, 256), 0) == key)
            b = one_hot(iota((128, 256), 0) == slot - head * 128)
            r = dot_nt(a, b).astype(BF16)
            row = pl.multiple_of(g * 16, 16)
            for h in range(32):
                counts[h // 8, pl.ds(row, 16), (h % 8) * 128 : (h % 8 + 1) * 128] = r[h * 16 : (h + 1) * 16]
            return 0

        lax.fori_loop(0, 32, group, 0)

    def build_sel(t):
        def group(g, _):
            sel[t, g] = one_hot(iota((1024, 256), 0) == place[t, g, :1, :])
            return 0

        lax.fori_loop(0, GROUPS, group, 0)

    def build_flush_plan(t):
        def group(g, _):
            s = sel[t, g]
            mix[g] = dot(counts[g], s).T.astype(BF16)
            base[g] = joined(dot_tn(s, parts(waiting[pl.ds(pl.multiple_of(g * 1024, 1024), 1024), :])))
            return 0

        lax.fori_loop(0, GROUPS, group, 0)

    def pooled_base(masked_by):
        total = jnp.zeros((BAGS, 2 * W), F32)
        for g in range(GROUPS):
            c = cache[g * 1024 : (g + 1) * 1024, :]
            if masked_by is not None:
                gone = dot(sel[masked_by, g], jnp.ones((256, W), BF16))
                c = jnp.where(gone > 0.5, 0.0, c)
            total = total + dot(counts[g], parts(c))
        return joined(total)

    def build_pick(t_prev):
        def group(g, _):
            pick[g] = dot(counts[g], sel[t_prev, g]).astype(BF16)
            return 0

        lax.fori_loop(0, GROUPS, group, 0)

    def update_waiting(t):
        def group(g, _):
            at = pl.ds(pl.multiple_of(g * 1024, 1024), 1024)
            w = waiting[at, :] + joined(dot_tn(counts[g], bag_grad[...]))
            gone = dot(sel[t, g], jnp.ones((256, W), BF16))
            waiting[at, :] = jnp.where(gone > 0.5, 0.0, w)
            return 0

        lax.fori_loop(0, GROUPS, group, 0)

    def update_cache(t):
        def group(g, _):
            at = pl.ds(pl.multiple_of(g * 1024, 1024), 1024)
            s = sel[t, g]
            new = joined(dot(s, freshp[g]))
            gone = dot(s, jnp.ones((256, W), BF16))
            cache[at, :] = jnp.where(gone > 0.5, new, cache[at, :])
            return 0

        lax.fori_loop(0, GROUPS, group, 0)

    def exchange_start(src, dst, send_sem, recv_sem):
        def one(k, _):
            p, target = partner(k)
            pltpu.make_async_remote_copy(
                src_ref=src.at[p], dst_ref=dst.at[me], send_sem=send_sem, recv_sem=recv_sem,
                device_id=target, device_id_type=MESH,
            ).start()
            return 0

        lax.fori_loop(1, N, one, 0)
        dst[me] = src[me]

    def exchange_wait(src, dst, send_sem, recv_sem):
        all_of = pltpu.make_async_remote_copy(
            src_ref=src.at[pl.ds(0, N - 1)], dst_ref=dst.at[pl.ds(0, N - 1)], send_sem=send_sem,
            recv_sem=recv_sem, device_id=partner(1)[1], device_id_type=MESH,
        )
        all_of.wait_send()
        all_of.wait_recv()

    def owner_plan(t):
        x = jnp.broadcast_to(idx_recv[...], (N, CAP, W)).reshape(N * CAP, W)
        e = iota((N * CAP, W), 0)
        mine = iota((N * CAP, W), 1) == t * CAP + e % CAP
        col = jnp.sum(jnp.where(mine, x, 0).astype(F32), axis=1, keepdims=True)
        wide = jnp.broadcast_to(col, (N * CAP, W))
        ycol[...] = wide.astype(I32)
        for b in range(8):
            turned = wide[b * 128 : (b + 1) * 128, :].T
            yrow[:, b * 128 : (b + 1) * 128] = turned[:8, :].astype(I32)
        y = yrow[:1, :]

        def chunk(c, _):
            at = pl.ds(pl.multiple_of(c * 256, 256), 256)
            m = one_hot(ycol[at, :1] == y)
            same[at, :] = m
            share[at, :] = 1.0 / dot(m, jnp.ones((1024, W), BF16))
            return 0

        lax.fori_loop(0, 4, chunk, 0)
        yc = ycol[...]
        head = yc // 128
        hot = one_hot(iota((N * CAP, W), 1) == head)[:, :64]
        a = accum_out[...]
        a1 = a.astype(BF16)
        a2 = (a - a1.astype(F32)).astype(BF16)
        a3 = (a - a1.astype(F32) - a2.astype(F32)).astype(BF16)
        got = dot(hot, a1) + dot(hot, a2) + dot(hot, a3)
        got = jnp.where(iota((N * CAP, W), 1) == yc - head * 128, got, 0.0)
        acc = jnp.sum(got, axis=1, keepdims=True)
        acc_old[...] = jnp.broadcast_to(jnp.where(yc[:, :1] < 0, 1.0, acc), (N * CAP, W))

        def fetch(src, _):
            for k in range(CAP):
                i = jnp.clip(idx_sm[src, 0, t * CAP + k], 0, ROWS - 1)
                old[src, k : k + 1, :] = table[pl.ds(i, 1), :]
            return 0

        lax.fori_loop(0, N, fetch, 0)

    def owner_update(t):
        got = parts(recv_f[t].reshape(N * CAP, W))
        total = joined(dot(same[...], got))
        extra = jnp.mean(total * total, axis=1, keepdims=True)
        acc = acc_old[...] + extra
        step = LEARN_RATE * total / jnp.sqrt(acc)
        send_b[t] = (old[...].reshape(N * CAP, W) - step).reshape(N, CAP, W)
        delta[:, :W] = step * share[...]
        delta[:, W:] = extra * share[...]

    def owner_store(t):
        y = yrow[:1, :]
        step = parts(delta[:, :W])

        def chunk(c, _):
            at = pl.ds(pl.multiple_of(c * 1024, 1024), 1024)
            hot = one_hot(iota((1024, 1024), 0) + c * 1024 == y)
            table[at, :] = table[at, :] - joined(dot(hot, step))
            return 0

        lax.fori_loop(0, ROWS // 1024, chunk, 0)
        yc = ycol[...]
        head = yc // 128
        tail = jnp.where(iota((N * CAP, W), 1) == yc - head * 128, delta[:, W:], 0.0)
        hot = one_hot(iota((64, N * CAP), 0) == y // 128)
        accum_out[...] = accum_out[...] + joined(dot(hot, parts(tail)))

    accum_out[...] = accum_ref[...]
    build_counts(0)
    pl.semaphore_wait(barrier, N - 1)
    exchange_start(idx_send, idx_recv, isend_sem.at[0], irecv_sem.at[0])
    build_sel(0)
    loads[0].wait()
    pooled = pooled_base(None)
    loads[2].wait()
    build_flush_plan(0)
    loads[1].wait()
    inv_copy.wait()
    for t in range(STEPS):
        if t > 0:
            pooled = base_pooled
            for g in range(GROUPS):
                pooled = pooled + joined(dot(pick[g], freshp[g]))
        grad = (pooled * (1.0 / BAG) - targets[t]) * (1.0 / BAG)
        bag_grad[...] = parts(grad)
        for g in range(GROUPS):
            out = base[g] + joined(dot(mix[g], bag_grad[...]))
            flush[g * 32 : (g + 1) * 32] = out.reshape(32, CAP, W)

        def to_owner(o, _):
            send_f[t, o] = flush[jnp.clip(inv_sm[0, o], 0, N - 1)]
            return 0

        lax.fori_loop(0, N, to_owner, 0, unroll=8)
        exchange_start(send_f.at[t], recv_f.at[t], fsend_sem.at[t], frecv_sem.at[t])
        update_waiting(t)
        if t == STEPS - 1:
            pending_store = pltpu.make_async_copy(waiting, pending_out, out_sem.at[0])
            pending_store.start()
        if t == 0:
            exchange_wait(idx_send, idx_recv, isend_sem.at[0], irecv_sem.at[0])
            idx_copy = pltpu.make_async_copy(idx_recv, idx_sm, sm_sem.at[1])
            idx_copy.start()
            loads[3].wait()
            idx_copy.wait()
        owner_plan(t)
        if t > 0:
            update_cache(t - 1)
        if t < STEPS - 1:
            build_counts(t + 1)
        exchange_wait(send_f.at[t], recv_f.at[t], fsend_sem.at[t], frecv_sem.at[t])
        owner_update(t)
        exchange_start(send_b.at[t], recv_b.at[t], bsend_sem.at[t], brecv_sem.at[t])
        if t < STEPS - 1:
            build_sel(t + 1)
            build_pick(t)
            base_pooled = pooled_base(t)
            build_flush_plan(t + 1)
        owner_store(t)
        if t == STEPS - 1:
            table_store = pltpu.make_async_copy(table, table_out, out_sem.at[1])
            table_store.start()
        exchange_wait(send_b.at[t], recv_b.at[t], bsend_sem.at[t], brecv_sem.at[t])

        def from_owner(j, _):
            fresh[j] = recv_b[t, jnp.clip(owner_sm[j], 0, N - 1)]
            return 0

        lax.fori_loop(0, N, from_owner, 0, unroll=8)
        for g in range(GROUPS):
            freshp[g] = parts(fresh[g * 32 : (g + 1) * 32].reshape(256, W))
    update_cache(STEPS - 1)
    cache_store = pltpu.make_async_copy(cache, cache_out, out_sem.at[2])
    cache_store.start()
    pending_store.wait()
    table_store.wait()
    cache_store.wait()


def body(table, accum, cache_values, cache_rows, pending, batch_slots, targets, dirty):
    keys = batch_slots.reshape(STEPS, 32, 256)
    rows = cache_rows.reshape(N, BLOCK)
    owners = rows[:, 0] // ROWS
    vmem = pl.BlockSpec(memory_space=pltpu.VMEM)
    smem = pl.BlockSpec(memory_space=pltpu.SMEM)
    hbm = pl.BlockSpec(memory_space=pl.ANY)
    dma = pltpu.SemaphoreType.DMA
    tiles = (N, CAP, W)
    new_table, new_accum, new_cache, new_pending = pl.pallas_call(
        kernel,
        out_shape=(
            jax.ShapeDtypeStruct((ROWS, W), F32),
            jax.ShapeDtypeStruct((64, W), F32),
            jax.ShapeDtypeStruct((SLOTS, W), F32),
            jax.ShapeDtypeStruct((SLOTS, W), F32),
        ),
        in_specs=[smem, vmem, vmem, vmem, vmem, hbm, hbm, hbm, hbm],
        out_specs=(hbm, vmem, hbm, hbm),
        scratch_shapes=[
            pltpu.VMEM((ROWS, W), F32),
            pltpu.VMEM((SLOTS, W), F32),
            pltpu.VMEM((SLOTS, W), F32),
            pltpu.VMEM((STEPS, BAGS, W), F32),
            pltpu.VMEM((GROUPS, BAGS, 1024), BF16),
            pltpu.VMEM((STEPS, GROUPS, 1024, 256), BF16),
            pltpu.VMEM((GROUPS, 256, BAGS), BF16),
            pltpu.VMEM((GROUPS, BAGS, 256), BF16),
            pltpu.VMEM((GROUPS, 256, W), F32),
            pltpu.VMEM(tiles, F32),
            pltpu.VMEM(tiles, F32),
            pltpu.VMEM((GROUPS, 256, 2 * W), BF16),
            pltpu.VMEM((BAGS, 2 * W), BF16),
            pltpu.VMEM((STEPS, *tiles), F32),
            pltpu.VMEM((STEPS, *tiles), F32),
            pltpu.VMEM((STEPS, *tiles), F32),
            pltpu.VMEM((STEPS, *tiles), F32),
            pltpu.VMEM((N, 1, W), I32),
            pltpu.VMEM((N, 1, W), I32),
            pltpu.SMEM((N, 1, W), I32),
            pltpu.VMEM((8, N), I32),
            pltpu.SMEM((8, N), I32),
            pltpu.VMEM((STEPS, GROUPS, 8, 256), I32),
            pltpu.VMEM((N * CAP, W), I32),
            pltpu.VMEM((8, N * CAP), I32),
            pltpu.VMEM((N * CAP, N * CAP), BF16),
            pltpu.VMEM((N * CAP, W), F32),
            pltpu.VMEM(tiles, F32),
            pltpu.VMEM((N * CAP, W), F32),
            pltpu.VMEM((N * CAP, 2 * W), F32),
            dma((4,)),
            dma((2,)),
            dma((3,)),
            dma((1,)),
            dma((1,)),
            dma((STEPS,)),
            dma((STEPS,)),
            dma((STEPS,)),
            dma((STEPS,)),
        ],
        compiler_params=pltpu.CompilerParams(
            collective_id=0, has_side_effects=True, vmem_limit_bytes=56 * 1024 * 1024
        ),
    )(
        owners, keys, dirty, rows, accum.reshape(64, W), table, cache_values, pending, targets
    )
    return new_table, new_accum.reshape(-1), new_cache, new_pending


def solution(mesh):
    in_specs = (
        P(("gx", "gy"), None),
        P(("gx", "gy")),
        P(("gx", "gy"), None),
        P(("gx", "gy")),
        P(("gx", "gy"), None),
        P(None, ("gx", "gy"), None),
        P(None, ("gx", "gy"), None),
        P(None, ("gx", "gy")),
    )
    out_specs = (
        P(("gx", "gy"), None),
        P(("gx", "gy")),
        P(("gx", "gy"), None),
        P(("gx", "gy"), None),
    )
    return jax.shard_map(body, mesh=mesh, in_specs=in_specs, out_specs=out_specs, check_vma=False)
```

```python
import functools

import jax
import jax.numpy as jnp
from jax import lax
from jax.experimental import pallas as pl
from jax.experimental.pallas import tpu as pltpu
from jax.sharding import PartitionSpec as P

LEARN_RATE = 0.3
LOGICAL = pl.DeviceIdType.LOGICAL
F32, BF16, I32 = jnp.float32, jnp.bfloat16, jnp.int32

N = 128
CAP = 8
W = 128
SLOTS = 4096
BLOCK = 32
ROWS = 8192
BAGS = 512
BAG = 16
STEPS = 3
GROUPS = 4


def iota(shape, dim):
    return lax.broadcasted_iota(I32, shape, dim)


def one_hot(mask):
    return jnp.where(mask, 1.0, 0.0).astype(BF16)


def parts(x):
    hi = x.astype(BF16)
    return jnp.concatenate([hi, (x - hi.astype(F32)).astype(BF16)], axis=1)


def joined(y):
    return y[:, :W] + y[:, W:]


def dot(a, b):
    return jnp.dot(a, b, preferred_element_type=F32)


def dot_nt(a, b):
    return lax.dot_general(a, b, (((1,), (1,)), ((), ())), preferred_element_type=F32)


def dot_tn(a, b):
    return lax.dot_general(a, b, (((0,), (0,)), ((), ())), preferred_element_type=F32)


def exact_bf16(x):
    return x.astype(BF16)


def kernel(
    owner_sm, keys_ref, dirty_ref, rows_ref, accum_ref, table_hbm, cache_hbm, pending_hbm, targets_hbm,
    answers_out, idx_out, accum_out, cache_out, pending_out,
    table, cache, waiting, targets, counts, sel, mix, pick, base, flush, fresh, freshp, bag_grad,
    send_f, recv_f, send_b, recv_b, idx_send, idx_recv, idx_sm, inv_v, inv_sm,
    place, ycol, yrow, same, share, old, acc_old, gone, gotp, deltap, more,
    in_sem, sm_sem, out_sem, isend_sem, irecv_sem, fsend_sem, frecv_sem, bsend_sem, brecv_sem,
):
    gx, gy = lax.axis_index("gx"), lax.axis_index("gy")
    me = gx * 16 + gy

    quarter, inner_id = me // 32, lax.rem(me, 32)

    def partner(q, k):
        return lax.rem(quarter + q, 4) * 32 + lax.rem(inner_id + k, 32)

    loads = [
        pltpu.make_async_copy(cache_hbm, cache, in_sem.at[0]),
        pltpu.make_async_copy(targets_hbm, targets, in_sem.at[1]),
        pltpu.make_async_copy(pending_hbm, waiting, in_sem.at[2]),
        pltpu.make_async_copy(table_hbm, table, in_sem.at[3]),
    ]
    for load in loads:
        load.start()
    barrier = pltpu.get_barrier_semaphore()

    for q in range(4):

        def greet(k, _):
            pl.semaphore_signal(barrier, inc=1, device_id=partner(q, k), device_id_type=LOGICAL)
            return 0

        lax.fori_loop(0 if q else 1, 32, greet, 0)

    lane_i = iota((BLOCK, 256), 1)
    sub_i = iota((BLOCK, 256), 0)
    before = one_hot(sub_i < lane_i % BLOCK)
    spread = one_hot(sub_i == lane_i % BLOCK)
    rows = rows_ref[...]
    local = rows - (rows // ROWS) * ROWS
    local_hi = local // 128
    local_lo = local - local_hi * 128
    rep_hi = dot(exact_bf16(local_hi.astype(F32)), spread)
    rep_lo = dot(exact_bf16(local_lo.astype(F32)), spread)
    want = (iota((N, 256), 1) // BLOCK).astype(F32)
    inner = (iota((N, 256), 1) % BLOCK).astype(F32)
    found = jnp.zeros((N, W), F32)
    at_hi = jnp.zeros((N, W), F32)
    at_lo = jnp.zeros((N, W), F32)
    at_in = jnp.zeros((N, W), F32)
    for t in range(STEPS):
        d = dirty_ref[t : t + 1, :]
        blk = d // BLOCK
        hot_b = one_hot(iota((N, BAGS), 0) == blk)
        hot_i = one_hot(iota((BLOCK, BAGS), 0) == d - blk * BLOCK)
        listed = exact_bf16(dot_nt(hot_b, hot_i))
        rank = dot(listed, before)
        there = dot(listed, spread)
        chosen = jnp.where((rank == want) & (there > 0.5), 1.0, 0.0)
        gather = one_hot(iota((256, W), 0) // BLOCK + t * CAP == iota((256, W), 1))
        found = found + dot(exact_bf16(chosen), gather)
        at_hi = at_hi + dot(exact_bf16(chosen * rep_hi), gather)
        at_lo = at_lo + dot(exact_bf16(chosen * rep_lo), gather)
        at_in = at_in + dot(exact_bf16(chosen * inner), gather)
    owner_col = rows[:, :1] // ROWS
    perm = one_hot(owner_col == iota((N, N), 1))
    sent_found = dot_tn(perm, exact_bf16(found))
    sent_hi = dot_tn(perm, exact_bf16(at_hi))
    sent_lo = dot_tn(perm, exact_bf16(at_lo))
    sent = jnp.where(sent_found > 0.5, sent_hi * 128.0 + sent_lo, -1.0).astype(I32)
    idx_send[...] = sent.reshape(N, 1, W)
    block_row = exact_bf16(iota((8, N), 1).astype(F32))
    inv_v[...] = jnp.minimum(dot(block_row, perm), N - 1.0).astype(I32)
    inv_copy = pltpu.make_async_copy(inv_v, inv_sm, sm_sem.at[0])
    inv_copy.start()
    in_block = jnp.where(found > 0.5, at_in, -1.0)
    for t in range(STEPS):
        rep8 = one_hot(iota((W, 256), 0) == iota((W, 256), 1) % CAP + t * CAP)
        wide_in = dot(exact_bf16(in_block), rep8)
        for g in range(GROUPS):
            jj = iota((N, 256), 0) - g * 32
            here = jj == iota((N, 256), 1) // CAP
            part = exact_bf16(jnp.where(here, wide_in, 0.0))
            inside = dot(jnp.ones((8, N), BF16), part)
            offset = (iota((8, 256), 1) // CAP * BLOCK).astype(F32)
            place[t, g] = jnp.where(inside < -0.5, -1.0, inside + offset).astype(I32)

    def build_counts(t):
        def group(g, _):
            slot = keys_ref[t, pl.ds(g, 1), :]
            head = slot // 128
            key = head * 16 + iota((1, 256), 1) // BAG
            a = one_hot(iota((512, 256), 0) == key)
            b = one_hot(iota((128, 256), 0) == slot - head * 128)
            r = dot_nt(a, b).astype(BF16)
            row = pl.multiple_of(g * 16, 16)
            for h in range(32):
                counts[h // 8, pl.ds(row, 16), (h % 8) * 128 : (h % 8 + 1) * 128] = r[h * 16 : (h + 1) * 16]
            return 0

        lax.fori_loop(0, 32, group, 0, unroll=4)

    def build_sel(t):
        def group(g, _):
            s = one_hot(iota((1024, 256), 0) == place[t, g, :1, :])
            sel[t, g] = s
            gone[t, g] = dot(s, jnp.ones((256, W), BF16))
            return 0

        lax.fori_loop(0, GROUPS, group, 0)

    def build_flush_plan(t):
        def group(g, _):
            s = sel[t, g]
            mix[g] = dot(counts[g], s).astype(BF16).T
            base[g] = joined(dot_tn(s, parts(waiting[pl.ds(pl.multiple_of(g * 1024, 1024), 1024), :])))
            return 0

        lax.fori_loop(0, GROUPS, group, 0)

    def pooled_base(masked_by):
        total = jnp.zeros((BAGS, 2 * W), F32)
        for g in range(GROUPS):
            c = cache[g * 1024 : (g + 1) * 1024, :]
            if masked_by is not None:
                c = jnp.where(gone[masked_by, g] > 0.5, 0.0, c)
            total = total + dot(counts[g], parts(c))
        return joined(total)

    def build_pick(t_prev):
        def group(g, _):
            pick[g] = dot(counts[g], sel[t_prev, g]).astype(BF16)
            return 0

        lax.fori_loop(0, GROUPS, group, 0)

    def update_waiting(t):
        def group(g, _):
            at = pl.ds(pl.multiple_of(g * 1024, 1024), 1024)
            w = waiting[at, :] + joined(dot_tn(counts[g], bag_grad[...]))
            waiting[at, :] = jnp.where(gone[t, g] > 0.5, 0.0, w)
            return 0

        lax.fori_loop(0, GROUPS, group, 0)

    def update_cache(t):
        def group(g, _):
            at = pl.ds(pl.multiple_of(g * 1024, 1024), 1024)
            new = joined(dot(sel[t, g], freshp[g]))
            cache[at, :] = jnp.where(gone[t, g] > 0.5, new, cache[at, :])
            return 0

        lax.fori_loop(0, GROUPS, group, 0)

    def send_quarter(q, src, dst, send_sem, recv_sem):
        def one(k, _):
            p = partner(q, k)
            pltpu.make_async_remote_copy(
                src_ref=src.at[p], dst_ref=dst.at[me], send_sem=send_sem, recv_sem=recv_sem,
                device_id=p, device_id_type=LOGICAL,
            ).start()
            return 0

        lax.fori_loop(0 if q else 1, 32, one, 0)

    def exchange_start(src, dst, send_sem, recv_sem):
        for q in range(4):
            send_quarter(q, src, dst, send_sem, recv_sem)
        dst[me] = src[me]

    def exchange_wait(src, dst, send_sem, recv_sem):
        all_of = pltpu.make_async_remote_copy(
            src_ref=src.at[pl.ds(0, N - 1)], dst_ref=dst.at[pl.ds(0, N - 1)], send_sem=send_sem,
            recv_sem=recv_sem, device_id=partner(0, 1), device_id_type=LOGICAL,
        )
        all_of.wait_send()
        all_of.wait_recv()

    def plan_rows(t):
        x = jnp.broadcast_to(idx_recv[...], (N, CAP, W)).reshape(N * CAP, W)
        e = iota((N * CAP, W), 0)
        mine = iota((N * CAP, W), 1) == t * CAP + e % CAP
        col = jnp.sum(jnp.where(mine, x, 0).astype(F32), axis=1, keepdims=True)
        wide = jnp.broadcast_to(col, (N * CAP, W))
        ycol[t] = wide.astype(I32)
        for b in range(8):
            turned = wide[b * 128 : (b + 1) * 128, :].T
            yrow[t, :, b * 128 : (b + 1) * 128] = turned[:8, :].astype(I32)
        y = yrow[t, :1, :]

        def chunk(c, _):
            at = pl.ds(pl.multiple_of(c * 256, 256), 256)
            m = one_hot(ycol[t, at, :1] == y)
            same[at, :] = m
            share[at, :] = 1.0 / dot(m, jnp.ones((1024, W), BF16))
            return 0

        lax.fori_loop(0, 4, chunk, 0)

    def plan_values(t):
        yc = ycol[t]
        head = yc // 128
        hot = one_hot(iota((N * CAP, W), 1) == head)[:, :64]
        got = joined(dot(hot, parts(accum_out[...])))
        got = jnp.where(iota((N * CAP, W), 1) == yc - head * 128, got, 0.0)
        acc = jnp.sum(got, axis=1, keepdims=True)
        acc_old[...] = jnp.broadcast_to(jnp.where(yc[:, :1] < 0, 1.0, acc), (N * CAP, W))

        def fetch(src, _):
            for k in range(CAP):
                i = jnp.clip(idx_sm[src, 0, t * CAP + k], 0, ROWS - 1)
                old[pl.ds(src * CAP + k, 1), :] = table[pl.ds(i, 1), :]
            return 0

        lax.fori_loop(0, N, fetch, 0)
        if t > 0:

            def correct(c, _):
                at = pl.ds(pl.multiple_of(c * 256, 256), 256)
                moved = jnp.zeros((256, 2 * W), F32)
                for s in range(t):
                    m = one_hot(ycol[t, at, :1] == yrow[s, :1, :])
                    moved = moved + dot(m, deltap[s])
                old[at, :] = old[at, :] - joined(moved)
                return 0

            lax.fori_loop(0, 4, correct, 0)

    def owner_update(t):
        gotp[...] = parts(recv_f[t].reshape(N * CAP, W))
        for q in range(4):
            base_src = lax.rem(quarter + q, 4) * 32
            at = pl.ds(pl.multiple_of(base_src * CAP, 256), 256)
            total = joined(dot(same[at, :], gotp[...]))
            extra = jnp.mean(total * total, axis=1, keepdims=True)
            step = total * (LEARN_RATE * lax.rsqrt(acc_old[at, :] + extra))
            send_b[t, pl.ds(base_src, 32)] = (old[at, :] - step).reshape(32, CAP, W)
            deltap[t, at, :] = parts(step * share[at, :])
            more[at, :] = extra * share[at, :]
            send_quarter(q, send_b.at[t], recv_b.at[t], bsend_sem.at[t], brecv_sem.at[t])
        recv_b[t, me] = send_b[t, me]

    def accum_update(t):
        y = yrow[t, :1, :]
        yc = ycol[t]
        tail = jnp.where(iota((N * CAP, W), 1) == yc - yc // 128 * 128, more[...], 0.0)
        hot = one_hot(iota((64, N * CAP), 0) == y // 128)
        accum_out[...] = accum_out[...] + joined(dot(hot, parts(tail)))

    accum_out[...] = accum_ref[...]
    stores = []
    build_counts(0)
    pl.semaphore_wait(barrier, N - 1)
    exchange_start(idx_send, idx_recv, isend_sem.at[0], irecv_sem.at[0])
    build_sel(0)
    loads[0].wait()
    pooled = pooled_base(None)
    loads[2].wait()
    build_flush_plan(0)
    loads[1].wait()
    inv_copy.wait()
    for t in range(STEPS):
        if t > 0:
            pooled = base_pooled
            for g in range(GROUPS):
                pooled = pooled + joined(dot(pick[g], freshp[g]))
        grad = (pooled * (1.0 / BAG) - targets[t]) * (1.0 / BAG)
        bag_grad[...] = parts(grad)
        for g in range(GROUPS):
            out = base[g] + joined(dot(mix[g], bag_grad[...]))
            flush[g * 32 : (g + 1) * 32] = out.reshape(32, CAP, W)

        def to_owner(o, _):
            send_f[t, o] = flush[jnp.clip(inv_sm[0, o], 0, N - 1)]
            return 0

        lax.fori_loop(0, N, to_owner, 0, unroll=8)
        exchange_start(send_f.at[t], recv_f.at[t], fsend_sem.at[t], frecv_sem.at[t])
        update_waiting(t)
        if t == STEPS - 1:
            pending_store = pltpu.make_async_copy(waiting, pending_out, out_sem.at[0])
            pending_store.start()
            stores.append(pending_store)
        if t == 0:
            exchange_wait(idx_send, idx_recv, isend_sem.at[0], irecv_sem.at[0])
            idx_copy = pltpu.make_async_copy(idx_recv, idx_sm, sm_sem.at[1])
            idx_copy.start()
            plan_rows(0)
            loads[3].wait()
            idx_copy.wait()
        plan_values(t)
        if t > 0:
            update_cache(t - 1)
        if t < STEPS - 1:
            build_counts(t + 1)
        exchange_wait(send_f.at[t], recv_f.at[t], fsend_sem.at[t], frecv_sem.at[t])
        owner_update(t)
        if t < STEPS - 1:
            build_sel(t + 1)
            build_pick(t)
            base_pooled = pooled_base(t)
            build_flush_plan(t + 1)
            plan_rows(t + 1)
        accum_update(t)
        answers = pltpu.make_async_copy(send_b.at[t], answers_out.at[t], out_sem.at[2 + t])
        answers.start()
        stores.append(answers)
        if t == 0:
            idx_store = pltpu.make_async_copy(idx_recv, idx_out, out_sem.at[1])
            idx_store.start()
            stores.append(idx_store)
        exchange_wait(send_b.at[t], recv_b.at[t], bsend_sem.at[t], brecv_sem.at[t])

        def from_owner(j, _):
            fresh[j] = recv_b[t, jnp.clip(owner_sm[j], 0, N - 1)]
            return 0

        lax.fori_loop(0, N, from_owner, 0, unroll=8)
        for g in range(GROUPS):
            freshp[g] = parts(fresh[g * 32 : (g + 1) * 32].reshape(256, W))
    update_cache(STEPS - 1)
    cache_store = pltpu.make_async_copy(cache, cache_out, out_sem.at[5])
    cache_store.start()
    stores.append(cache_store)
    for store in stores:
        store.wait()


def finish(
    idx_sm, table_hbm, answers_hbm, cache_hbm, pending_hbm, table_out, cache_out, pending_out,
    table, answers, cache, pending, in_sem, out_sem,
):
    loads = [
        pltpu.make_async_copy(answers_hbm, answers, in_sem.at[0]),
        pltpu.make_async_copy(table_hbm, table.at[pl.ds(0, ROWS)], in_sem.at[1]),
        pltpu.make_async_copy(cache_hbm, cache, in_sem.at[2]),
        pltpu.make_async_copy(pending_hbm, pending, in_sem.at[3]),
    ]
    for load in loads:
        load.start()
    loads[2].wait()
    cache_store = pltpu.make_async_copy(cache, cache_out, out_sem.at[0])
    cache_store.start()
    loads[3].wait()
    pending_store = pltpu.make_async_copy(pending, pending_out, out_sem.at[1])
    pending_store.start()
    loads[0].wait()
    loads[1].wait()
    for t in range(STEPS):

        def rows_of(src, _):
            for k in range(CAP):
                i = idx_sm[src, 0, t * CAP + k]
                i = jnp.where(i < 0, ROWS, jnp.minimum(i, ROWS))
                table[pl.ds(i, 1), :] = answers[t, src, k : k + 1, :]
            return 0

        lax.fori_loop(0, N, rows_of, 0, unroll=2)
    table_store = pltpu.make_async_copy(table.at[pl.ds(0, ROWS)], table_out, out_sem.at[2])
    table_store.start()
    cache_store.wait()
    pending_store.wait()
    table_store.wait()


def body(table, accum, cache_values, cache_rows, pending, batch_slots, targets, dirty):
    keys = batch_slots.reshape(STEPS, 32, 256)
    rows = cache_rows.reshape(N, BLOCK)
    owners = rows[:, 0] // ROWS
    vmem = pl.BlockSpec(memory_space=pltpu.VMEM)
    smem = pl.BlockSpec(memory_space=pltpu.SMEM)
    hbm = pl.BlockSpec(memory_space=pl.ANY)
    dma = pltpu.SemaphoreType.DMA
    tiles = (N, CAP, W)
    answers, idx, new_accum, new_cache, new_pending = pl.pallas_call(
        kernel,
        out_shape=(
            jax.ShapeDtypeStruct((STEPS, *tiles), F32),
            jax.ShapeDtypeStruct((N, 1, W), I32),
            jax.ShapeDtypeStruct((64, W), F32),
            jax.ShapeDtypeStruct((SLOTS, W), F32),
            jax.ShapeDtypeStruct((SLOTS, W), F32),
        ),
        in_specs=[smem, vmem, vmem, vmem, vmem, hbm, hbm, hbm, hbm],
        out_specs=(hbm, hbm, vmem, hbm, hbm),
        scratch_shapes=[
            pltpu.VMEM((ROWS, W), F32),
            pltpu.VMEM((SLOTS, W), F32),
            pltpu.VMEM((SLOTS, W), F32),
            pltpu.VMEM((STEPS, BAGS, W), F32),
            pltpu.VMEM((GROUPS, BAGS, 1024), BF16),
            pltpu.VMEM((STEPS, GROUPS, 1024, 256), BF16),
            pltpu.VMEM((GROUPS, 256, BAGS), BF16),
            pltpu.VMEM((GROUPS, BAGS, 256), BF16),
            pltpu.VMEM((GROUPS, 256, W), F32),
            pltpu.VMEM(tiles, F32),
            pltpu.VMEM(tiles, F32),
            pltpu.VMEM((GROUPS, 256, 2 * W), BF16),
            pltpu.VMEM((BAGS, 2 * W), BF16),
            pltpu.VMEM((STEPS, *tiles), F32),
            pltpu.VMEM((STEPS, *tiles), F32),
            pltpu.VMEM((STEPS, *tiles), F32),
            pltpu.VMEM((STEPS, *tiles), F32),
            pltpu.VMEM((N, 1, W), I32),
            pltpu.VMEM((N, 1, W), I32),
            pltpu.SMEM((N, 1, W), I32),
            pltpu.VMEM((8, N), I32),
            pltpu.SMEM((8, N), I32),
            pltpu.VMEM((STEPS, GROUPS, 8, 256), I32),
            pltpu.VMEM((STEPS, N * CAP, W), I32),
            pltpu.VMEM((STEPS, 8, N * CAP), I32),
            pltpu.VMEM((N * CAP, N * CAP), BF16),
            pltpu.VMEM((N * CAP, W), F32),
            pltpu.VMEM((N * CAP, W), F32),
            pltpu.VMEM((N * CAP, W), F32),
            pltpu.VMEM((STEPS, GROUPS, 1024, W), F32),
            pltpu.VMEM((N * CAP, 2 * W), BF16),
            pltpu.VMEM((STEPS, N * CAP, 2 * W), BF16),
            pltpu.VMEM((N * CAP, W), F32),
            dma((4,)),
            dma((2,)),
            dma((6,)),
            dma((1,)),
            dma((1,)),
            dma((STEPS,)),
            dma((STEPS,)),
            dma((STEPS,)),
            dma((STEPS,)),
        ],
        compiler_params=pltpu.CompilerParams(
            collective_id=0, has_side_effects=True, vmem_limit_bytes=56 * 1024 * 1024
        ),
    )(
        owners, keys, dirty, rows, accum.reshape(64, W), table, cache_values, pending, targets
    )
    new_table, new_cache, new_pending = pl.pallas_call(
        finish,
        out_shape=(
            jax.ShapeDtypeStruct((ROWS, W), F32),
            jax.ShapeDtypeStruct((SLOTS, W), F32),
            jax.ShapeDtypeStruct((SLOTS, W), F32),
        ),
        in_specs=[smem, hbm, hbm, hbm, hbm],
        out_specs=(hbm, hbm, hbm),
        scratch_shapes=[
            pltpu.VMEM((ROWS + 8, W), F32),
            pltpu.VMEM((STEPS, *tiles), F32),
            pltpu.VMEM((SLOTS, W), F32),
            pltpu.VMEM((SLOTS, W), F32),
            dma((4,)),
            dma((3,)),
        ],
    )(idx, table, answers, new_cache, new_pending)
    return new_table, new_accum.reshape(-1), new_cache, new_pending


def solution(mesh):
    in_specs = (
        P(("gx", "gy"), None),
        P(("gx", "gy")),
        P(("gx", "gy"), None),
        P(("gx", "gy")),
        P(("gx", "gy"), None),
        P(None, ("gx", "gy"), None),
        P(None, ("gx", "gy"), None),
        P(None, ("gx", "gy")),
    )
    out_specs = (
        P(("gx", "gy"), None),
        P(("gx", "gy")),
        P(("gx", "gy"), None),
        P(("gx", "gy"), None),
    )
    return jax.shard_map(body, mesh=mesh, in_specs=in_specs, out_specs=out_specs, check_vma=False)
```

```python
import functools

import jax
import jax.numpy as jnp
from jax import lax
from jax.experimental import pallas as pl
from jax.experimental.pallas import tpu as pltpu
from jax.sharding import PartitionSpec as P

LEARN_RATE = 0.3
FAR_A, FAR_B, FAR_M = 6, 2, 9
LOGICAL = pl.DeviceIdType.LOGICAL
F32, BF16, I32 = jnp.float32, jnp.bfloat16, jnp.int32

N = 128
CAP = 8
W = 128
SLOTS = 4096
BLOCK = 32
ROWS = 8192
BAGS = 512
BAG = 16
STEPS = 3
GROUPS = 4


def iota(shape, dim):
    return lax.broadcasted_iota(I32, shape, dim)


def one_hot(mask):
    return jnp.where(mask, 1.0, 0.0).astype(BF16)


def parts(x):
    hi = x.astype(BF16)
    return jnp.concatenate([hi, (x - hi.astype(F32)).astype(BF16)], axis=1)


def joined(y):
    return y[:, :W] + y[:, W:]


def dot(a, b):
    return jnp.dot(a, b, preferred_element_type=F32)


def dot_nt(a, b):
    return lax.dot_general(a, b, (((1,), (1,)), ((), ())), preferred_element_type=F32)


def dot_tn(a, b):
    return lax.dot_general(a, b, (((0,), (0,)), ((), ())), preferred_element_type=F32)


def exact_bf16(x):
    return x.astype(BF16)


def kernel(
    held_sm, keys_ref, dirty_ref, rows_ref, accum_ref, table_hbm, cache_hbm, pending_hbm, targets_hbm,
    answers_out, idx_out, accum_out, cache_out, pending_out,
    table, cache, waiting, targets, counts, sel, mix, pick, base, flush, fresh, freshp, bag_grad,
    send_f, recv_f, send_b, recv_b, idx_send, idx_recv, idx_sm, inv_v, inv_sm,
    place, placec, ycol, yrow, same, share, old, acc_old, gone, gotp, deltap, more,
    in_sem, sm_sem, out_sem, isend_sem, irecv_sem, fsend_sem, frecv_sem, bsend_sem, brecv_sem,
):
    gx, gy = lax.axis_index("gx"), lax.axis_index("gy")
    me = gx * 16 + gy

    quarter, core, px, py = gx // 2, lax.rem(gx, 2), gy // 4, lax.rem(gy, 4)
    far = (2, 1, 3, 0)
    line = [lax.rem(core + 1 - c, 2) * 16 + lax.rem(py + dy, 4) for dy in far for c in range(2)]

    def each_partner(q, act):
        plane = lax.rem(quarter + q, 4) * 32

        def row(n, _):
            dx = lax.rem(FAR_A * n * n + FAR_B * n + 2, FAR_M)
            start = plane + lax.rem(px + dx, 4) * 4
            for p in line:
                act(start + p)
            return 0

        lax.fori_loop(0, 4 if q else 3, row, 0)
        if q == 0:
            for p in line[:-1]:
                act(plane + px * 4 + p)

    loads = [
        pltpu.make_async_copy(cache_hbm, cache, in_sem.at[0]),
        pltpu.make_async_copy(targets_hbm, targets, in_sem.at[1]),
        pltpu.make_async_copy(pending_hbm, waiting, in_sem.at[2]),
        pltpu.make_async_copy(table_hbm, table, in_sem.at[3]),
    ]
    for load in loads:
        load.start()
    barrier = pltpu.get_barrier_semaphore()

    for q in far:
        each_partner(q, lambda p: pl.semaphore_signal(barrier, inc=1, device_id=p, device_id_type=LOGICAL))

    lane_i = iota((BLOCK, 256), 1)
    sub_i = iota((BLOCK, 256), 0)
    before = one_hot(sub_i < lane_i % BLOCK)
    spread = one_hot(sub_i == lane_i % BLOCK)
    rows = rows_ref[...]
    local = rows - (rows // ROWS) * ROWS
    local_hi = local // 128
    local_lo = local - local_hi * 128
    rep_hi = dot(exact_bf16(local_hi.astype(F32)), spread)
    rep_lo = dot(exact_bf16(local_lo.astype(F32)), spread)
    want = (iota((N, 256), 1) // BLOCK).astype(F32)
    inner = (iota((N, 256), 1) % BLOCK).astype(F32)
    found = jnp.zeros((N, W), F32)
    at_hi = jnp.zeros((N, W), F32)
    at_lo = jnp.zeros((N, W), F32)
    at_in = jnp.zeros((N, W), F32)
    for t in range(STEPS):
        d = dirty_ref[t : t + 1, :]
        blk = d // BLOCK
        hot_b = one_hot(iota((N, BAGS), 0) == blk)
        hot_i = one_hot(iota((BLOCK, BAGS), 0) == d - blk * BLOCK)
        listed = exact_bf16(dot_nt(hot_b, hot_i))
        rank = dot(listed, before)
        there = dot(listed, spread)
        chosen = jnp.where((rank == want) & (there > 0.5), 1.0, 0.0)
        gather = one_hot(iota((256, W), 0) // BLOCK + t * CAP == iota((256, W), 1))
        found = found + dot(exact_bf16(chosen), gather)
        at_hi = at_hi + dot(exact_bf16(chosen * rep_hi), gather)
        at_lo = at_lo + dot(exact_bf16(chosen * rep_lo), gather)
        at_in = at_in + dot(exact_bf16(chosen * inner), gather)
    owner_col = rows[:, :1] // ROWS
    perm = one_hot(owner_col == iota((N, N), 1))
    sent_found = dot_tn(perm, exact_bf16(found))
    sent_hi = dot_tn(perm, exact_bf16(at_hi))
    sent_lo = dot_tn(perm, exact_bf16(at_lo))
    sent = jnp.where(sent_found > 0.5, sent_hi * 128.0 + sent_lo, float(ROWS)).astype(I32)
    idx_send[...] = sent.reshape(N, 1, W)
    block_row = exact_bf16(iota((8, N), 1).astype(F32))
    inv_v[...] = jnp.minimum(dot(block_row, perm), N - 1.0).astype(I32)
    inv_copy = pltpu.make_async_copy(inv_v, inv_sm, sm_sem.at[0])
    inv_copy.start()
    in_block = jnp.where(found > 0.5, at_in, -1.0)
    for t in range(STEPS):
        rep8 = one_hot(iota((W, 256), 0) == iota((W, 256), 1) % CAP + t * CAP)
        wide_in = dot(exact_bf16(in_block), rep8)
        for g in range(GROUPS):
            jj = iota((N, 256), 0) - g * 32
            here = jj == iota((N, 256), 1) // CAP
            part = exact_bf16(jnp.where(here, wide_in, 0.0))
            inside = dot(jnp.ones((8, N), BF16), part)
            offset = (iota((8, 256), 1) // CAP * BLOCK).astype(F32)
            place[t, g] = jnp.where(inside < -0.5, -1.0, inside + offset).astype(I32)
            inside = dot_tn(part, jnp.ones((N, W), BF16))
            offset = (iota((256, W), 0) // CAP * BLOCK).astype(F32)
            placec[t, g] = jnp.where(inside < -0.5, -1.0, inside + offset).astype(I32)

    def build_counts(t):
        def group(g, _):
            slot = keys_ref[t, pl.ds(g, 1), :]
            head = slot // 128
            key = head * 16 + iota((1, 256), 1) // BAG
            a = one_hot(iota((512, 256), 0) == key)
            b = one_hot(iota((128, 256), 0) == slot - head * 128)
            r = dot_nt(a, b).astype(BF16)
            row = pl.multiple_of(g * 16, 16)
            for h in range(32):
                counts[h // 8, pl.ds(row, 16), (h % 8) * 128 : (h % 8 + 1) * 128] = r[h * 16 : (h + 1) * 16]
            return 0

        lax.fori_loop(0, 32, group, 0, unroll=8)

    def build_sel(t):
        def group(g, _):
            s = one_hot(iota((1024, 256), 0) == place[t, g, :1, :])
            sel[t, g] = s
            gone[t, g] = dot(s, jnp.ones((256, W), BF16))
            return 0

        lax.fori_loop(0, GROUPS, group, 0, unroll=2)

    def build_flush_plan(t):
        def group(g, _):
            s = sel[t, g]
            mix[g] = dot(counts[g], s).astype(BF16).T
            st = one_hot(iota((256, 1024), 1) == placec[t, g, :, :1])
            base[g] = joined(dot(st, parts(waiting[pl.ds(pl.multiple_of(g * 1024, 1024), 1024), :])))
            return 0

        lax.fori_loop(0, GROUPS, group, 0, unroll=2)

    def pooled_base(masked_by):
        total = jnp.zeros((BAGS, 2 * W), F32)
        for g in range(GROUPS):
            c = cache[g * 1024 : (g + 1) * 1024, :]
            if masked_by is not None:
                c = jnp.where(gone[masked_by, g] > 0.5, 0.0, c)
            total = total + dot(counts[g], parts(c))
        return joined(total)

    def build_pick(t_prev):
        def group(g, _):
            pick[g] = dot(counts[g], sel[t_prev, g]).astype(BF16)
            return 0

        lax.fori_loop(0, GROUPS, group, 0, unroll=2)

    def update_waiting(t):
        def group(g, _):
            at = pl.ds(pl.multiple_of(g * 1024, 1024), 1024)
            w = waiting[at, :] + joined(dot_tn(counts[g], bag_grad[...]))
            waiting[at, :] = jnp.where(gone[t, g] > 0.5, 0.0, w)
            return 0

        lax.fori_loop(0, GROUPS, group, 0, unroll=2)

    def update_cache(t):
        def group(g, _):
            at = pl.ds(pl.multiple_of(g * 1024, 1024), 1024)
            new = joined(dot(sel[t, g], freshp[g]))
            cache[at, :] = jnp.where(gone[t, g] > 0.5, new, cache[at, :])
            return 0

        lax.fori_loop(0, GROUPS, group, 0, unroll=2)

    def send_quarter(q, src, dst, send_sem, recv_sem):
        def one(p):
            pltpu.make_async_remote_copy(
                src_ref=src.at[p], dst_ref=dst.at[me], send_sem=send_sem, recv_sem=recv_sem,
                device_id=p, device_id_type=LOGICAL,
            ).start()

        each_partner(q, one)

    def exchange_start(src, dst, send_sem, recv_sem):
        for q in far:
            send_quarter(q, src, dst, send_sem, recv_sem)
        dst[me] = src[me]

    def exchange_wait(src, dst, send_sem, recv_sem):
        all_of = pltpu.make_async_remote_copy(
            src_ref=src.at[pl.ds(0, N - 1)], dst_ref=dst.at[pl.ds(0, N - 1)], send_sem=send_sem,
            recv_sem=recv_sem, device_id=lax.rem(me + 1, N), device_id_type=LOGICAL,
        )
        all_of.wait_send()
        all_of.wait_recv()

    def plan_rows(t):
        x = jnp.broadcast_to(idx_recv[...], (N, CAP, W)).reshape(N * CAP, W)
        e = iota((N * CAP, W), 0)
        mine = iota((N * CAP, W), 1) == t * CAP + e % CAP
        col = jnp.sum(jnp.where(mine, x, 0).astype(F32), axis=1, keepdims=True)
        wide = jnp.broadcast_to(col, (N * CAP, W))
        ycol[t] = wide.astype(I32)
        for b in range(8):
            turned = wide[b * 128 : (b + 1) * 128, :].T
            yrow[t, :, b * 128 : (b + 1) * 128] = turned[:8, :].astype(I32)
        y = yrow[t, :1, :]

        def chunk(c, _):
            at = pl.ds(pl.multiple_of(c * 256, 256), 256)
            m = one_hot(ycol[t, at, :1] == y)
            same[at, :] = m
            share[at, :] = 1.0 / dot(m, jnp.ones((1024, W), BF16))
            return 0

        lax.fori_loop(0, 4, chunk, 0, unroll=2)

    def plan_values(t):
        yc = ycol[t]
        head = yc // 128
        hot = one_hot(iota((N * CAP, W), 1) == head)[:, :64]
        got = joined(dot(hot, parts(accum_out[...])))
        got = jnp.where(iota((N * CAP, W), 1) == yc - head * 128, got, 0.0)
        acc = jnp.sum(got, axis=1, keepdims=True)
        acc_old[...] = jnp.broadcast_to(jnp.where(yc[:, :1] >= ROWS, 1.0, acc), (N * CAP, W))

        def fetch(src, _):
            for k in range(CAP):
                i = jnp.clip(idx_sm[src, 0, t * CAP + k], 0, ROWS - 1)
                old[pl.ds(src * CAP + k, 1), :] = table[pl.ds(i, 1), :]
            return 0

        lax.fori_loop(0, N, fetch, 0, unroll=4)
        if t > 0:

            def correct(c, _):
                at = pl.ds(pl.multiple_of(c * 256, 256), 256)
                moved = jnp.zeros((256, 2 * W), F32)
                for s in range(t):
                    m = one_hot(ycol[t, at, :1] == yrow[s, :1, :])
                    moved = moved + dot(m, deltap[s])
                old[at, :] = old[at, :] - joined(moved)
                return 0

            lax.fori_loop(0, 4, correct, 0, unroll=2)

    def owner_update(t):
        gotp[...] = parts(recv_f[t].reshape(N * CAP, W))
        for q in far:
            base_src = lax.rem(quarter + q, 4) * 32
            at = pl.ds(pl.multiple_of(base_src * CAP, 256), 256)
            total = joined(dot(same[at, :], gotp[...]))
            extra = jnp.mean(total * total, axis=1, keepdims=True)
            step = total * (LEARN_RATE * lax.rsqrt(acc_old[at, :] + extra))
            send_b[t, pl.ds(base_src, 32)] = (old[at, :] - step).reshape(32, CAP, W)
            deltap[t, at, :] = parts(step * share[at, :])
            more[at, :] = extra * share[at, :]
            send_quarter(q, send_b.at[t], recv_b.at[t], bsend_sem.at[t], brecv_sem.at[t])
        recv_b[t, me] = send_b[t, me]

    def accum_update(t):
        y = yrow[t, :1, :]
        yc = ycol[t]
        tail = jnp.where(iota((N * CAP, W), 1) == yc - yc // 128 * 128, more[...], 0.0)
        hot = one_hot(iota((64, N * CAP), 0) == y // 128)
        accum_out[...] = accum_out[...] + joined(dot(hot, parts(tail)))

    accum_out[...] = accum_ref[...]
    stores = []
    build_counts(0)
    pl.semaphore_wait(barrier, N - 1)
    exchange_start(idx_send, idx_recv, isend_sem.at[0], irecv_sem.at[0])
    build_sel(0)
    loads[0].wait()
    pooled = pooled_base(None)
    loads[2].wait()
    build_flush_plan(0)
    loads[1].wait()
    inv_copy.wait()
    for t in range(STEPS):
        if t > 0:
            moved = dot(pick[0], freshp[0])
            for g in range(1, GROUPS):
                moved = moved + dot(pick[g], freshp[g])
            pooled = base_pooled + joined(moved)
        grad = (pooled * (1.0 / BAG) - targets[t]) * (1.0 / BAG)
        bag_grad[...] = parts(grad)
        for g in range(GROUPS):
            out = base[g] + joined(dot(mix[g], bag_grad[...]))
            flush[g * 32 : (g + 1) * 32] = out.reshape(32, CAP, W)

        for n, q in enumerate((*far, None)):
            if q is not None:
                first = lax.rem(quarter + q, 4) * 32

                def to_owner(o, _):
                    send_f[t, first + o] = flush[jnp.clip(inv_sm[0, first + o], 0, N - 1)]
                    return 0

                lax.fori_loop(0, 32, to_owner, 0, unroll=8)
            if n > 0:
                send_quarter(far[n - 1], send_f.at[t], recv_f.at[t], fsend_sem.at[t], frecv_sem.at[t])
        recv_f[t, me] = send_f[t, me]
        update_waiting(t)
        if t == STEPS - 1:
            pending_store = pltpu.make_async_copy(waiting, pending_out, out_sem.at[0])
            pending_store.start()
            stores.append(pending_store)
        if t == 0:
            exchange_wait(idx_send, idx_recv, isend_sem.at[0], irecv_sem.at[0])
            idx_copy = pltpu.make_async_copy(idx_recv, idx_sm, sm_sem.at[1])
            idx_copy.start()
            plan_rows(0)
            loads[3].wait()
            idx_copy.wait()
        plan_values(t)
        if t > 0:
            update_cache(t - 1)
        if t < STEPS - 1:
            build_counts(t + 1)
        exchange_wait(send_f.at[t], recv_f.at[t], fsend_sem.at[t], frecv_sem.at[t])
        owner_update(t)
        if t < STEPS - 1:
            build_sel(t + 1)
            build_pick(t)
            base_pooled = pooled_base(t)
            build_flush_plan(t + 1)
            plan_rows(t + 1)
        accum_update(t)
        answers = pltpu.make_async_copy(send_b.at[t], answers_out.at[t], out_sem.at[2 + t])
        answers.start()
        stores.append(answers)
        if t == 0:
            idx_store = pltpu.make_async_copy(idx_recv, idx_out, out_sem.at[1])
            idx_store.start()
            stores.append(idx_store)
        exchange_wait(send_b.at[t], recv_b.at[t], bsend_sem.at[t], brecv_sem.at[t])

        def from_owner(j, _):
            fresh[j] = recv_b[t, jnp.clip(lax.div(held_sm[j * BLOCK], ROWS), 0, N - 1)]
            return 0

        lax.fori_loop(0, N, from_owner, 0, unroll=8)
        for g in range(GROUPS):
            freshp[g] = parts(fresh[g * 32 : (g + 1) * 32].reshape(256, W))
    update_cache(STEPS - 1)
    cache_store = pltpu.make_async_copy(cache, cache_out, out_sem.at[5])
    cache_store.start()
    stores.append(cache_store)
    for store in stores:
        store.wait()


def finish(
    idx_sm, table_hbm, answers_hbm, cache_hbm, pending_hbm, table_out, cache_out, pending_out,
    table, answers, cache, pending, in_sem, out_sem,
):
    loads = [
        pltpu.make_async_copy(answers_hbm, answers, in_sem.at[0]),
        pltpu.make_async_copy(table_hbm, table.at[pl.ds(0, ROWS)], in_sem.at[1]),
        pltpu.make_async_copy(cache_hbm, cache, in_sem.at[2]),
        pltpu.make_async_copy(pending_hbm, pending, in_sem.at[3]),
    ]
    for load in loads:
        load.start()
    loads[2].wait()
    cache_store = pltpu.make_async_copy(cache, cache_out, out_sem.at[0])
    cache_store.start()
    loads[3].wait()
    pending_store = pltpu.make_async_copy(pending, pending_out, out_sem.at[1])
    pending_store.start()
    loads[0].wait()
    loads[1].wait()
    for t in range(STEPS):

        def rows_of(src, _):
            for k in range(CAP):
                table[pl.ds(idx_sm[src, 0, t * CAP + k], 1), :] = answers[t, src, k : k + 1, :]
            return 0

        lax.fori_loop(0, N, rows_of, 0, unroll=4)
    table_store = pltpu.make_async_copy(table.at[pl.ds(0, ROWS)], table_out, out_sem.at[2])
    table_store.start()
    cache_store.wait()
    pending_store.wait()
    table_store.wait()


def body(table, accum, cache_values, cache_rows, pending, batch_slots, targets, dirty):
    keys = batch_slots.reshape(STEPS, 32, 256)
    rows = cache_rows.reshape(N, BLOCK)
    vmem = pl.BlockSpec(memory_space=pltpu.VMEM)
    smem = pl.BlockSpec(memory_space=pltpu.SMEM)
    hbm = pl.BlockSpec(memory_space=pl.ANY)
    dma = pltpu.SemaphoreType.DMA
    tiles = (N, CAP, W)
    answers, idx, new_accum, new_cache, new_pending = pl.pallas_call(
        kernel,
        out_shape=(
            jax.ShapeDtypeStruct((STEPS, *tiles), F32),
            jax.ShapeDtypeStruct((N, 1, W), I32),
            jax.ShapeDtypeStruct((64, W), F32),
            jax.ShapeDtypeStruct((SLOTS, W), F32),
            jax.ShapeDtypeStruct((SLOTS, W), F32),
        ),
        in_specs=[smem, vmem, vmem, vmem, vmem, hbm, hbm, hbm, hbm],
        out_specs=(hbm, hbm, vmem, hbm, hbm),
        scratch_shapes=[
            pltpu.VMEM((ROWS, W), F32),
            pltpu.VMEM((SLOTS, W), F32),
            pltpu.VMEM((SLOTS, W), F32),
            pltpu.VMEM((STEPS, BAGS, W), F32),
            pltpu.VMEM((GROUPS, BAGS, 1024), BF16),
            pltpu.VMEM((STEPS, GROUPS, 1024, 256), BF16),
            pltpu.VMEM((GROUPS, 256, BAGS), BF16),
            pltpu.VMEM((GROUPS, BAGS, 256), BF16),
            pltpu.VMEM((GROUPS, 256, W), F32),
            pltpu.VMEM(tiles, F32),
            pltpu.VMEM(tiles, F32),
            pltpu.VMEM((GROUPS, 256, 2 * W), BF16),
            pltpu.VMEM((BAGS, 2 * W), BF16),
            pltpu.VMEM((STEPS, *tiles), F32),
            pltpu.VMEM((STEPS, *tiles), F32),
            pltpu.VMEM((STEPS, *tiles), F32),
            pltpu.VMEM((STEPS, *tiles), F32),
            pltpu.VMEM((N, 1, W), I32),
            pltpu.VMEM((N, 1, W), I32),
            pltpu.SMEM((N, 1, W), I32),
            pltpu.VMEM((8, N), I32),
            pltpu.SMEM((8, N), I32),
            pltpu.VMEM((STEPS, GROUPS, 8, 256), I32),
            pltpu.VMEM((STEPS, GROUPS, 256, W), I32),
            pltpu.VMEM((STEPS, N * CAP, W), I32),
            pltpu.VMEM((STEPS, 8, N * CAP), I32),
            pltpu.VMEM((N * CAP, N * CAP), BF16),
            pltpu.VMEM((N * CAP, W), F32),
            pltpu.VMEM((N * CAP, W), F32),
            pltpu.VMEM((N * CAP, W), F32),
            pltpu.VMEM((STEPS, GROUPS, 1024, W), F32),
            pltpu.VMEM((N * CAP, 2 * W), BF16),
            pltpu.VMEM((STEPS, N * CAP, 2 * W), BF16),
            pltpu.VMEM((N * CAP, W), F32),
            dma((4,)),
            dma((2,)),
            dma((6,)),
            dma((1,)),
            dma((1,)),
            dma((STEPS,)),
            dma((STEPS,)),
            dma((STEPS,)),
            dma((STEPS,)),
        ],
        compiler_params=pltpu.CompilerParams(
            collective_id=0, has_side_effects=True, vmem_limit_bytes=56 * 1024 * 1024
        ),
    )(
        cache_rows, keys, dirty, rows, accum.reshape(64, W), table, cache_values, pending, targets
    )
    new_table, new_cache, new_pending = pl.pallas_call(
        finish,
        out_shape=(
            jax.ShapeDtypeStruct((ROWS, W), F32),
            jax.ShapeDtypeStruct((SLOTS, W), F32),
            jax.ShapeDtypeStruct((SLOTS, W), F32),
        ),
        in_specs=[smem, hbm, hbm, hbm, hbm],
        out_specs=(hbm, hbm, hbm),
        scratch_shapes=[
            pltpu.VMEM((ROWS + 8, W), F32),
            pltpu.VMEM((STEPS, *tiles), F32),
            pltpu.VMEM((SLOTS, W), F32),
            pltpu.VMEM((SLOTS, W), F32),
            dma((4,)),
            dma((3,)),
        ],
    )(idx, table, answers, new_cache, new_pending)
    return new_table, new_accum.reshape(-1), new_cache, new_pending


def solution(mesh):
    in_specs = (
        P(("gx", "gy"), None),
        P(("gx", "gy")),
        P(("gx", "gy"), None),
        P(("gx", "gy")),
        P(("gx", "gy"), None),
        P(None, ("gx", "gy"), None),
        P(None, ("gx", "gy"), None),
        P(None, ("gx", "gy")),
    )
    out_specs = (
        P(("gx", "gy"), None),
        P(("gx", "gy")),
        P(("gx", "gy"), None),
        P(("gx", "gy"), None),
    )
    return jax.shard_map(body, mesh=mesh, in_specs=in_specs, out_specs=out_specs, check_vma=False)
```

```python
import functools

import jax
import jax.numpy as jnp
from jax import lax
from jax.experimental import pallas as pl
from jax.experimental.pallas import tpu as pltpu
from jax.sharding import PartitionSpec as P

LEARN_RATE = 0.3
FAR_A, FAR_B, FAR_M = 6, 2, 9
LOGICAL = pl.DeviceIdType.LOGICAL
F32, BF16, I32 = jnp.float32, jnp.bfloat16, jnp.int32

N = 128
CAP = 8
W = 128
SLOTS = 4096
BLOCK = 32
ROWS = 8192
BAGS = 512
BAG = 16
STEPS = 3
GROUPS = 4


def iota(shape, dim):
    return lax.broadcasted_iota(I32, shape, dim)


def one_hot(mask):
    return jnp.where(mask, 1.0, 0.0).astype(BF16)


def parts(x):
    hi = x.astype(BF16)
    return jnp.concatenate([hi, (x - hi.astype(F32)).astype(BF16)], axis=1)


def joined(y):
    return y[:, :W] + y[:, W:]


def dot(a, b):
    return jnp.dot(a, b, preferred_element_type=F32)


def dot_nt(a, b):
    return lax.dot_general(a, b, (((1,), (1,)), ((), ())), preferred_element_type=F32)


def dot_tn(a, b):
    return lax.dot_general(a, b, (((0,), (0,)), ((), ())), preferred_element_type=F32)


def exact_bf16(x):
    return x.astype(BF16)


def kernel(
    held_hbm, keys_ref, dirty_ref, rows_ref, accum_ref, table_hbm, cache_hbm, pending_hbm, targets_hbm,
    answers_out, idx_out, accum_out, cache_out, pending_out,
    table, cache, waiting, targets, counts, sel, mix, pick, base, flush, fresh, freshp, bag_grad,
    send_f, recv_f, send_b, recv_b, idx_send, idx_recv, idx_sm, inv_v, inv_sm, held_sm,
    in_block, place, placec, ycol, yrow, same, share, old, acc_old, gone, gotp, deltap, more,
    in_sem, sm_sem, out_sem, isend_sem, irecv_sem, fsend_sem, frecv_sem, bsend_sem, brecv_sem,
):
    gx, gy = lax.axis_index("gx"), lax.axis_index("gy")
    me = gx * 16 + gy

    quarter, core, px, py = gx // 2, lax.rem(gx, 2), gy // 4, lax.rem(gy, 4)
    far = (2, 1, 3, 0)
    line = [lax.rem(core + 1 - c, 2) * 16 + lax.rem(py + dy, 4) for dy in far for c in range(2)]

    def each_partner(q, act):
        plane = lax.rem(quarter + q, 4) * 32

        def row(n, _):
            dx = lax.rem(FAR_A * n * n + FAR_B * n + 2, FAR_M)
            start = plane + lax.rem(px + dx, 4) * 4
            for p in line:
                act(start + p)
            return 0

        lax.fori_loop(0, 4 if q else 3, row, 0)
        if q == 0:
            for p in line[:-1]:
                act(plane + px * 4 + p)

    loads = [
        pltpu.make_async_copy(cache_hbm, cache, in_sem.at[0]),
        pltpu.make_async_copy(targets_hbm, targets, in_sem.at[1]),
        pltpu.make_async_copy(pending_hbm, waiting, in_sem.at[2]),
        pltpu.make_async_copy(table_hbm, table, in_sem.at[3]),
        pltpu.make_async_copy(held_hbm, held_sm, in_sem.at[4]),
    ]
    for load in loads:
        load.start()
    barrier = pltpu.get_barrier_semaphore()

    for q in far:
        each_partner(q, lambda p: pl.semaphore_signal(barrier, inc=1, device_id=p, device_id_type=LOGICAL))

    lane_i = iota((BLOCK, 256), 1)
    sub_i = iota((BLOCK, 256), 0)
    before = one_hot(sub_i < lane_i % BLOCK)
    spread = one_hot(sub_i == lane_i % BLOCK)
    rows = rows_ref[...]
    owner = rows // ROWS
    local = rows - owner * ROWS
    local_hi = local // 128
    local_lo = local - local_hi * 128
    lift = one_hot(iota((N, 32), 1) == iota((N, 32), 0) // 4)
    lane, part_of = iota((N, W), 1), iota((N, W), 0) % 4
    fold = one_hot(iota((W, 256), 0) % BLOCK == iota((W, 256), 1) % BLOCK)

    def lifted(x, keep):
        return jnp.where(keep, dot(lift, exact_bf16(x.astype(F32))), 0.0)

    rep_hi = dot(exact_bf16(lifted(local_hi, lane // BLOCK == part_of)), fold)
    rep_lo = dot(exact_bf16(lifted(local_lo, lane // BLOCK == part_of)), fold)
    owner_col = jnp.sum(lifted(owner, lane == part_of * BLOCK), axis=1, keepdims=True).astype(I32)
    want = (iota((N, 256), 1) // BLOCK).astype(F32)
    inner = (iota((N, 256), 1) % BLOCK).astype(F32)
    found = jnp.zeros((N, W), F32)
    at_hi = jnp.zeros((N, W), F32)
    at_lo = jnp.zeros((N, W), F32)
    at_in = jnp.zeros((N, W), F32)
    for t in range(STEPS):
        d = dirty_ref[t : t + 1, :]
        blk = d // BLOCK
        hot_b = one_hot(iota((N, BAGS), 0) == blk)
        hot_i = one_hot(iota((BLOCK, BAGS), 0) == d - blk * BLOCK)
        listed = exact_bf16(dot_nt(hot_b, hot_i))
        rank = dot(listed, before)
        there = dot(listed, spread)
        chosen = jnp.where((rank == want) & (there > 0.5), 1.0, 0.0)
        gather = one_hot(iota((256, W), 0) // BLOCK + t * CAP == iota((256, W), 1))
        found = found + dot(exact_bf16(chosen), gather)
        at_hi = at_hi + dot(exact_bf16(chosen * rep_hi), gather)
        at_lo = at_lo + dot(exact_bf16(chosen * rep_lo), gather)
        at_in = at_in + dot(exact_bf16(chosen * inner), gather)
    perm = one_hot(owner_col == iota((N, N), 1))
    sent_found = dot_tn(perm, exact_bf16(found))
    sent_hi = dot_tn(perm, exact_bf16(at_hi))
    sent_lo = dot_tn(perm, exact_bf16(at_lo))
    sent = jnp.where(sent_found > 0.5, sent_hi * 128.0 + sent_lo, float(ROWS)).astype(I32)
    idx_send[...] = sent.reshape(N, 1, W)
    block_row = exact_bf16(iota((8, N), 1).astype(F32))
    inv_v[...] = jnp.minimum(dot(block_row, perm), N - 1.0).astype(I32)
    inv_copy = pltpu.make_async_copy(inv_v, inv_sm, sm_sem.at[0])
    inv_copy.start()
    in_block[...] = jnp.where(found > 0.5, at_in, -1.0)

    def build_counts(t):
        def group(g, _):
            slot = keys_ref[t, pl.ds(g, 1), :]
            head = slot // 128
            key = head * 16 + iota((1, 256), 1) // BAG
            a = one_hot(iota((512, 256), 0) == key)
            b = one_hot(iota((128, 256), 0) == slot - head * 128)
            r = dot_nt(a, b).astype(BF16)
            row = pl.multiple_of(g * 16, 16)
            for h in range(32):
                counts[h // 8, pl.ds(row, 16), (h % 8) * 128 : (h % 8 + 1) * 128] = r[h * 16 : (h + 1) * 16]
            return 0

        lax.fori_loop(0, 32, group, 0, unroll=8)

    def build_place(t):
        rep8 = one_hot(iota((W, 256), 0) == iota((W, 256), 1) % CAP + t * CAP)
        wide_in = dot(exact_bf16(in_block[...]), rep8)
        for g in range(GROUPS):
            jj = iota((N, 256), 0) - g * 32
            here = jj == iota((N, 256), 1) // CAP
            part = exact_bf16(jnp.where(here, wide_in, 0.0))
            inside = dot(jnp.ones((8, N), BF16), part)
            offset = (iota((8, 256), 1) // CAP * BLOCK).astype(F32)
            place[g] = jnp.where(inside < -0.5, -1.0, inside + offset).astype(I32)
            inside = dot_tn(part, jnp.ones((N, W), BF16))
            offset = (iota((256, W), 0) // CAP * BLOCK).astype(F32)
            placec[g] = jnp.where(inside < -0.5, -1.0, inside + offset).astype(I32)

    def build_sel(t):
        build_place(t)

        def group(g, _):
            s = one_hot(iota((1024, 256), 0) == place[g, :1, :])
            sel[t, g] = s
            gone[t, g] = dot(s, jnp.ones((256, W), BF16))
            return 0

        lax.fori_loop(0, GROUPS, group, 0, unroll=2)

    def build_flush_plan(t):
        def group(g, _):
            s = sel[t, g]
            mix[g] = dot(counts[g], s).astype(BF16).T
            st = one_hot(iota((256, 1024), 1) == placec[g, :, :1])
            base[g] = joined(dot(st, parts(waiting[pl.ds(pl.multiple_of(g * 1024, 1024), 1024), :])))
            return 0

        lax.fori_loop(0, GROUPS, group, 0, unroll=2)

    def pooled_base(masked_by):
        total = jnp.zeros((BAGS, 2 * W), F32)
        for g in range(GROUPS):
            c = cache[g * 1024 : (g + 1) * 1024, :]
            if masked_by is not None:
                c = jnp.where(gone[masked_by, g] > 0.5, 0.0, c)
            total = total + dot(counts[g], parts(c))
        return joined(total)

    def build_pick(t_prev):
        def group(g, _):
            pick[g] = dot(counts[g], sel[t_prev, g]).astype(BF16)
            return 0

        lax.fori_loop(0, GROUPS, group, 0, unroll=2)

    def update_waiting(t):
        def group(g, _):
            at = pl.ds(pl.multiple_of(g * 1024, 1024), 1024)
            w = waiting[at, :] + joined(dot_tn(counts[g], bag_grad[...]))
            waiting[at, :] = jnp.where(gone[t, g] > 0.5, 0.0, w)
            return 0

        lax.fori_loop(0, GROUPS, group, 0, unroll=2)

    def update_cache(t):
        def group(g, _):
            at = pl.ds(pl.multiple_of(g * 1024, 1024), 1024)
            new = joined(dot(sel[t, g], freshp[g]))
            cache[at, :] = jnp.where(gone[t, g] > 0.5, new, cache[at, :])
            return 0

        lax.fori_loop(0, GROUPS, group, 0, unroll=2)

    def send_quarter(q, src, dst, send_sem, recv_sem):
        def one(p):
            pltpu.make_async_remote_copy(
                src_ref=src.at[p], dst_ref=dst.at[me], send_sem=send_sem, recv_sem=recv_sem,
                device_id=p, device_id_type=LOGICAL,
            ).start()

        each_partner(q, one)

    def exchange_start(src, dst, send_sem, recv_sem):
        for q in far:
            send_quarter(q, src, dst, send_sem, recv_sem)
        dst[me] = src[me]

    def exchange_wait(src, dst, send_sem, recv_sem):
        all_of = pltpu.make_async_remote_copy(
            src_ref=src.at[pl.ds(0, N - 1)], dst_ref=dst.at[pl.ds(0, N - 1)], send_sem=send_sem,
            recv_sem=recv_sem, device_id=lax.rem(me + 1, N), device_id_type=LOGICAL,
        )
        all_of.wait_send()
        all_of.wait_recv()

    def plan_rows(t):
        x = jnp.broadcast_to(idx_recv[...], (N, CAP, W)).reshape(N * CAP, W)
        e = iota((N * CAP, W), 0)
        mine = iota((N * CAP, W), 1) == t * CAP + e % CAP
        col = jnp.sum(jnp.where(mine, x, 0).astype(F32), axis=1, keepdims=True)
        wide = jnp.broadcast_to(col, (N * CAP, W))
        ycol[t] = wide.astype(I32)
        for b in range(8):
            turned = wide[b * 128 : (b + 1) * 128, :].T
            yrow[t, :, b * 128 : (b + 1) * 128] = turned[:8, :].astype(I32)
        y = yrow[t, :1, :]

        def chunk(c, _):
            at = pl.ds(pl.multiple_of(c * 256, 256), 256)
            m = one_hot(ycol[t, at, :1] == y)
            same[at, :] = m
            share[at, :] = 1.0 / dot(m, jnp.ones((1024, W), BF16))
            return 0

        lax.fori_loop(0, 4, chunk, 0, unroll=2)

    def plan_values(t):
        yc = ycol[t]
        head = yc // 128
        hot = one_hot(iota((N * CAP, W), 1) == head)[:, :64]
        got = joined(dot(hot, parts(accum_out[...])))
        got = jnp.where(iota((N * CAP, W), 1) == yc - head * 128, got, 0.0)
        acc = jnp.sum(got, axis=1, keepdims=True)
        acc_old[...] = jnp.broadcast_to(jnp.where(yc[:, :1] >= ROWS, 1.0, acc), (N * CAP, W))

        def fetch(src, _):
            for k in range(CAP):
                i = jnp.clip(idx_sm[src, 0, t * CAP + k], 0, ROWS - 1)
                old[pl.ds(src * CAP + k, 1), :] = table[pl.ds(i, 1), :]
            return 0

        lax.fori_loop(0, N, fetch, 0, unroll=4)
        if t > 0:

            def correct(c, _):
                at = pl.ds(pl.multiple_of(c * 256, 256), 256)
                moved = jnp.zeros((256, 2 * W), F32)
                for s in range(t):
                    m = one_hot(ycol[t, at, :1] == yrow[s, :1, :])
                    moved = moved + dot(m, deltap[s])
                old[at, :] = old[at, :] - joined(moved)
                return 0

            lax.fori_loop(0, 4, correct, 0, unroll=2)

    def owner_update(t):
        gotp[...] = parts(recv_f[t].reshape(N * CAP, W))
        for q in far:
            base_src = lax.rem(quarter + q, 4) * 32
            at = pl.ds(pl.multiple_of(base_src * CAP, 256), 256)
            total = joined(dot(same[at, :], gotp[...]))
            extra = jnp.mean(total * total, axis=1, keepdims=True)
            step = total * (LEARN_RATE * lax.rsqrt(acc_old[at, :] + extra))
            send_b[t, pl.ds(base_src, 32)] = (old[at, :] - step).reshape(32, CAP, W)
            deltap[t, at, :] = parts(step * share[at, :])
            more[at, :] = extra * share[at, :]
            send_quarter(q, send_b.at[t], recv_b.at[t], bsend_sem.at[t], brecv_sem.at[t])
        recv_b[t, me] = send_b[t, me]

    def accum_update(t):
        y = yrow[t, :1, :]
        yc = ycol[t]
        tail = jnp.where(iota((N * CAP, W), 1) == yc - yc // 128 * 128, more[...], 0.0)
        hot = one_hot(iota((64, N * CAP), 0) == y // 128)
        accum_out[...] = accum_out[...] + joined(dot(hot, parts(tail)))

    accum_out[...] = accum_ref[...]
    stores = []
    build_counts(0)
    pl.semaphore_wait(barrier, N - 1)
    exchange_start(idx_send, idx_recv, isend_sem.at[0], irecv_sem.at[0])
    build_sel(0)
    loads[0].wait()
    pooled = pooled_base(None)
    loads[2].wait()
    build_flush_plan(0)
    loads[1].wait()
    inv_copy.wait()
    for t in range(STEPS):
        if t > 0:
            moved = dot(pick[0], freshp[0])
            for g in range(1, GROUPS):
                moved = moved + dot(pick[g], freshp[g])
            pooled = base_pooled + joined(moved)
        grad = (pooled * (1.0 / BAG) - targets[t]) * (1.0 / BAG)
        bag_grad[...] = parts(grad)
        for g in range(GROUPS):
            out = base[g] + joined(dot(mix[g], bag_grad[...]))
            flush[g * 32 : (g + 1) * 32] = out.reshape(32, CAP, W)

        for n, q in enumerate((*far, None)):
            if q is not None:
                first = lax.rem(quarter + q, 4) * 32

                def to_owner(o, _):
                    send_f[t, first + o] = flush[jnp.clip(inv_sm[0, first + o], 0, N - 1)]
                    return 0

                lax.fori_loop(0, 32, to_owner, 0, unroll=8)
            if n > 0:
                send_quarter(far[n - 1], send_f.at[t], recv_f.at[t], fsend_sem.at[t], frecv_sem.at[t])
        recv_f[t, me] = send_f[t, me]
        update_waiting(t)
        if t == STEPS - 1:
            pending_store = pltpu.make_async_copy(waiting, pending_out, out_sem.at[0])
            pending_store.start()
            stores.append(pending_store)
        if t == 0:
            exchange_wait(idx_send, idx_recv, isend_sem.at[0], irecv_sem.at[0])
            idx_copy = pltpu.make_async_copy(idx_recv, idx_sm, sm_sem.at[1])
            idx_copy.start()
            plan_rows(0)
            loads[3].wait()
            loads[4].wait()
            idx_copy.wait()
        plan_values(t)
        if t > 0:
            update_cache(t - 1)
        if t < STEPS - 1:
            build_counts(t + 1)
        exchange_wait(send_f.at[t], recv_f.at[t], fsend_sem.at[t], frecv_sem.at[t])
        owner_update(t)
        if t < STEPS - 1:
            build_sel(t + 1)
            build_pick(t)
            base_pooled = pooled_base(t)
            build_flush_plan(t + 1)
            plan_rows(t + 1)
        accum_update(t)
        answers = pltpu.make_async_copy(send_b.at[t], answers_out.at[t], out_sem.at[2 + t])
        answers.start()
        stores.append(answers)
        if t == 0:
            idx_store = pltpu.make_async_copy(idx_recv, idx_out, out_sem.at[1])
            idx_store.start()
            stores.append(idx_store)
        exchange_wait(send_b.at[t], recv_b.at[t], bsend_sem.at[t], brecv_sem.at[t])

        def from_owner(j, _):
            fresh[j] = recv_b[t, jnp.clip(lax.div(held_sm[j * BLOCK], ROWS), 0, N - 1)]
            return 0

        lax.fori_loop(0, N, from_owner, 0, unroll=8)
        for g in range(GROUPS):
            freshp[g] = parts(fresh[g * 32 : (g + 1) * 32].reshape(256, W))
    update_cache(STEPS - 1)
    cache_store = pltpu.make_async_copy(cache, cache_out, out_sem.at[5])
    cache_store.start()
    stores.append(cache_store)
    for store in stores:
        store.wait()


def finish(
    idx_hbm, accum_in, table_hbm, answers_hbm, cache_hbm, pending_hbm,
    accum_out, table_out, cache_out, pending_out,
    table, answers, cache, pending, idx_sm, in_sem, out_sem,
):
    loads = [
        pltpu.make_async_copy(answers_hbm, answers, in_sem.at[0]),
        pltpu.make_async_copy(table_hbm, table.at[pl.ds(0, ROWS)], in_sem.at[1]),
        pltpu.make_async_copy(cache_hbm, cache, in_sem.at[2]),
        pltpu.make_async_copy(pending_hbm, pending, in_sem.at[3]),
        pltpu.make_async_copy(idx_hbm, idx_sm, in_sem.at[4]),
    ]
    loads[4].start()
    loads[0].start()
    loads[1].start()
    accum_out[...] = accum_in[...]
    loads[0].wait()
    loads[1].wait()
    loads[2].start()
    loads[3].start()
    loads[4].wait()
    for t in range(STEPS):

        def rows_of(src, _):
            for k in range(CAP):
                table[pl.ds(idx_sm[src, 0, t * CAP + k], 1), :] = answers[t, src, k : k + 1, :]
            return 0

        lax.fori_loop(0, N, rows_of, 0, unroll=4)
        if t == 0:
            loads[2].wait()
            cache_store = pltpu.make_async_copy(cache, cache_out, out_sem.at[0])
            cache_store.start()
            loads[3].wait()
            pending_store = pltpu.make_async_copy(pending, pending_out, out_sem.at[1])
            pending_store.start()
    table_store = pltpu.make_async_copy(table.at[pl.ds(0, ROWS)], table_out, out_sem.at[2])
    table_store.start()
    cache_store.wait()
    pending_store.wait()
    table_store.wait()


def body(table, accum, cache_values, cache_rows, pending, batch_slots, targets, dirty):
    keys = batch_slots.reshape(STEPS, 32, 256)
    rows = cache_rows.reshape(32, 128)
    vmem = pl.BlockSpec(memory_space=pltpu.VMEM)
    hbm = pl.BlockSpec(memory_space=pl.ANY)
    dma = pltpu.SemaphoreType.DMA
    tiles = (N, CAP, W)
    answers, idx, new_accum, new_cache, new_pending = pl.pallas_call(
        kernel,
        out_shape=(
            jax.ShapeDtypeStruct((STEPS, *tiles), F32),
            jax.ShapeDtypeStruct((N, 1, W), I32),
            jax.ShapeDtypeStruct((64, W), F32),
            jax.ShapeDtypeStruct((SLOTS, W), F32),
            jax.ShapeDtypeStruct((SLOTS, W), F32),
        ),
        in_specs=[hbm, vmem, vmem, vmem, vmem, hbm, hbm, hbm, hbm],
        out_specs=(hbm, hbm, vmem, hbm, hbm),
        scratch_shapes=[
            pltpu.VMEM((ROWS, W), F32),
            pltpu.VMEM((SLOTS, W), F32),
            pltpu.VMEM((SLOTS, W), F32),
            pltpu.VMEM((STEPS, BAGS, W), F32),
            pltpu.VMEM((GROUPS, BAGS, 1024), BF16),
            pltpu.VMEM((STEPS, GROUPS, 1024, 256), BF16),
            pltpu.VMEM((GROUPS, 256, BAGS), BF16),
            pltpu.VMEM((GROUPS, BAGS, 256), BF16),
            pltpu.VMEM((GROUPS, 256, W), F32),
            pltpu.VMEM(tiles, F32),
            pltpu.VMEM(tiles, F32),
            pltpu.VMEM((GROUPS, 256, 2 * W), BF16),
            pltpu.VMEM((BAGS, 2 * W), BF16),
            pltpu.VMEM((STEPS, *tiles), F32),
            pltpu.VMEM((STEPS, *tiles), F32),
            pltpu.VMEM((STEPS, *tiles), F32),
            pltpu.VMEM((STEPS, *tiles), F32),
            pltpu.VMEM((N, 1, W), I32),
            pltpu.VMEM((N, 1, W), I32),
            pltpu.SMEM((N, 1, W), I32),
            pltpu.VMEM((8, N), I32),
            pltpu.SMEM((8, N), I32),
            pltpu.SMEM((SLOTS,), I32),
            pltpu.VMEM((N, W), F32),
            pltpu.VMEM((GROUPS, 8, 256), I32),
            pltpu.VMEM((GROUPS, 256, W), I32),
            pltpu.VMEM((STEPS, N * CAP, W), I32),
            pltpu.VMEM((STEPS, 8, N * CAP), I32),
            pltpu.VMEM((N * CAP, N * CAP), BF16),
            pltpu.VMEM((N * CAP, W), F32),
            pltpu.VMEM((N * CAP, W), F32),
            pltpu.VMEM((N * CAP, W), F32),
            pltpu.VMEM((STEPS, GROUPS, 1024, W), F32),
            pltpu.VMEM((N * CAP, 2 * W), BF16),
            pltpu.VMEM((STEPS, N * CAP, 2 * W), BF16),
            pltpu.VMEM((N * CAP, W), F32),
            dma((5,)),
            dma((2,)),
            dma((6,)),
            dma((1,)),
            dma((1,)),
            dma((STEPS,)),
            dma((STEPS,)),
            dma((STEPS,)),
            dma((STEPS,)),
        ],
        compiler_params=pltpu.CompilerParams(
            collective_id=0, has_side_effects=True, vmem_limit_bytes=56 * 1024 * 1024
        ),
    )(
        cache_rows, keys, dirty, rows, accum.reshape(64, W), table, cache_values, pending, targets
    )
    new_accum, new_table, new_cache, new_pending = pl.pallas_call(
        finish,
        out_shape=(
            jax.ShapeDtypeStruct((64, W), F32),
            jax.ShapeDtypeStruct((ROWS, W), F32),
            jax.ShapeDtypeStruct((SLOTS, W), F32),
            jax.ShapeDtypeStruct((SLOTS, W), F32),
        ),
        in_specs=[hbm, vmem, hbm, hbm, hbm, hbm],
        out_specs=(vmem, hbm, hbm, hbm),
        scratch_shapes=[
            pltpu.VMEM((ROWS + 8, W), F32),
            pltpu.VMEM((STEPS, *tiles), F32),
            pltpu.VMEM((SLOTS, W), F32),
            pltpu.VMEM((SLOTS, W), F32),
            pltpu.SMEM((N, 1, W), I32),
            dma((5,)),
            dma((3,)),
        ],
    )(idx, new_accum, table, answers, new_cache, new_pending)
    return new_table, new_accum.reshape(-1), new_cache, new_pending


def solution(mesh):
    in_specs = (
        P(("gx", "gy"), None),
        P(("gx", "gy")),
        P(("gx", "gy"), None),
        P(("gx", "gy")),
        P(("gx", "gy"), None),
        P(None, ("gx", "gy"), None),
        P(None, ("gx", "gy"), None),
        P(None, ("gx", "gy")),
    )
    out_specs = (
        P(("gx", "gy"), None),
        P(("gx", "gy")),
        P(("gx", "gy"), None),
        P(("gx", "gy"), None),
    )
    return jax.shard_map(body, mesh=mesh, in_specs=in_specs, out_specs=out_specs, check_vma=False)
```

```python
import functools

import jax
import jax.numpy as jnp
from jax import lax
from jax.experimental import pallas as pl
from jax.experimental.pallas import tpu as pltpu
from jax.sharding import PartitionSpec as P

LEARN_RATE = 0.3
FAR_A, FAR_B, FAR_M = 6, 2, 9
LOGICAL = pl.DeviceIdType.LOGICAL
F32, BF16, I32 = jnp.float32, jnp.bfloat16, jnp.int32

N = 128
CAP = 8
W = 128
SLOTS = 4096
BLOCK = 32
ROWS = 8192
BAGS = 512
BAG = 16
STEPS = 3
GROUPS = 4


def iota(shape, dim):
    return lax.broadcasted_iota(I32, shape, dim)


def one_hot(mask):
    return jnp.where(mask, 1.0, 0.0).astype(BF16)


def parts(x):
    hi = x.astype(BF16)
    return jnp.concatenate([hi, (x - hi.astype(F32)).astype(BF16)], axis=1)


def joined(y):
    return y[:, :W] + y[:, W:]


def dot(a, b):
    return jnp.dot(a, b, preferred_element_type=F32)


def dot_nt(a, b):
    return lax.dot_general(a, b, (((1,), (1,)), ((), ())), preferred_element_type=F32)


def dot_tn(a, b):
    return lax.dot_general(a, b, (((0,), (0,)), ((), ())), preferred_element_type=F32)


def exact_bf16(x):
    return x.astype(BF16)


def kernel(
    held_hbm, keys_ref, dirty_ref, rows_ref, accum_ref, table_hbm, cache_hbm, pending_hbm, targets_hbm,
    answers_out, idx_out, accum_out, cache_out, pending_out,
    table, cache, waiting, targets, counts, sel, mix, pick, base, flush, fresh, freshp, bag_grad,
    send_f, recv_f, send_b, recv_b, idx_send, idx_recv, idx_sm, inv_v, inv_sm, held_sm,
    in_block, place, placec, ycol, yrow, same, share, old, acc_old, gone, gotp, deltap, more,
    in_sem, sm_sem, out_sem, isend_sem, irecv_sem, fsend_sem, frecv_sem, bsend_sem, brecv_sem,
):
    gx, gy = lax.axis_index("gx"), lax.axis_index("gy")
    me = gx * 16 + gy

    quarter, core, px, py = gx // 2, lax.rem(gx, 2), gy // 4, lax.rem(gy, 4)
    far = (2, 1, 3, 0)
    line = [lax.rem(core + 1 - c, 2) * 16 + lax.rem(py + dy, 4) for dy in far for c in range(2)]

    def each_partner(q, act):
        plane = lax.rem(quarter + q, 4) * 32

        def row(n, _):
            dx = lax.rem(FAR_A * n * n + FAR_B * n + 2, FAR_M)
            start = plane + lax.rem(px + dx, 4) * 4
            for p in line:
                act(start + p)
            return 0

        lax.fori_loop(0, 4 if q else 3, row, 0)
        if q == 0:
            for p in line[:-1]:
                act(plane + px * 4 + p)

    loads = [
        pltpu.make_async_copy(cache_hbm, cache, in_sem.at[0]),
        pltpu.make_async_copy(targets_hbm, targets, in_sem.at[1]),
        pltpu.make_async_copy(pending_hbm, waiting, in_sem.at[2]),
        pltpu.make_async_copy(table_hbm, table, in_sem.at[3]),
        pltpu.make_async_copy(held_hbm, held_sm, in_sem.at[4]),
    ]
    for load in loads:
        load.start()
    barrier = pltpu.get_barrier_semaphore()

    for q in far:
        each_partner(q, lambda p: pl.semaphore_signal(barrier, inc=1, device_id=p, device_id_type=LOGICAL))

    lane_i = iota((BLOCK, 256), 1)
    sub_i = iota((BLOCK, 256), 0)
    before = one_hot(sub_i < lane_i % BLOCK)
    spread = one_hot(sub_i == lane_i % BLOCK)
    rows = rows_ref[...]
    owner = rows // ROWS
    local = rows - owner * ROWS
    local_hi = local // 128
    local_lo = local - local_hi * 128
    lift = one_hot(iota((N, 32), 1) == iota((N, 32), 0) // 4)
    lane, part_of = iota((N, W), 1), iota((N, W), 0) % 4
    fold = one_hot(iota((W, 256), 0) % BLOCK == iota((W, 256), 1) % BLOCK)

    def lifted(x, keep):
        return jnp.where(keep, dot(lift, exact_bf16(x.astype(F32))), 0.0)

    rep_hi = dot(exact_bf16(lifted(local_hi, lane // BLOCK == part_of)), fold)
    rep_lo = dot(exact_bf16(lifted(local_lo, lane // BLOCK == part_of)), fold)
    owner_col = jnp.sum(lifted(owner, lane == part_of * BLOCK), axis=1, keepdims=True).astype(I32)
    want = (iota((N, 256), 1) // BLOCK).astype(F32)
    inner = (iota((N, 256), 1) % BLOCK).astype(F32)
    found = jnp.zeros((N, W), F32)
    at_hi = jnp.zeros((N, W), F32)
    at_lo = jnp.zeros((N, W), F32)
    at_in = jnp.zeros((N, W), F32)
    for t in range(STEPS):
        d = dirty_ref[t : t + 1, :]
        blk = d // BLOCK
        hot_b = one_hot(iota((N, BAGS), 0) == blk)
        hot_i = one_hot(iota((BLOCK, BAGS), 0) == d - blk * BLOCK)
        listed = exact_bf16(dot_nt(hot_b, hot_i))
        rank = dot(listed, before)
        there = dot(listed, spread)
        chosen = jnp.where((rank == want) & (there > 0.5), 1.0, 0.0)
        gather = one_hot(iota((256, W), 0) // BLOCK + t * CAP == iota((256, W), 1))
        found = found + dot(exact_bf16(chosen), gather)
        at_hi = at_hi + dot(exact_bf16(chosen * rep_hi), gather)
        at_lo = at_lo + dot(exact_bf16(chosen * rep_lo), gather)
        at_in = at_in + dot(exact_bf16(chosen * inner), gather)
    perm = one_hot(owner_col == iota((N, N), 1))
    sent_found = dot_tn(perm, exact_bf16(found))
    sent_hi = dot_tn(perm, exact_bf16(at_hi))
    sent_lo = dot_tn(perm, exact_bf16(at_lo))
    sent = jnp.where(sent_found > 0.5, sent_hi * 128.0 + sent_lo, float(ROWS)).astype(I32)
    idx_send[...] = sent.reshape(N, 1, W)
    block_row = exact_bf16(iota((8, N), 1).astype(F32))
    inv_v[...] = jnp.minimum(dot(block_row, perm), N - 1.0).astype(I32)
    inv_copy = pltpu.make_async_copy(inv_v, inv_sm, sm_sem.at[0])
    inv_copy.start()
    in_block[...] = jnp.where(found > 0.5, at_in, -1.0)

    def build_counts(t):
        def group(g, _):
            slot = keys_ref[t, pl.ds(g, 1), :]
            head = slot // 128
            key = head * 16 + iota((1, 256), 1) // BAG
            a = one_hot(iota((512, 256), 0) == key)
            b = one_hot(iota((128, 256), 0) == slot - head * 128)
            r = dot_nt(a, b).astype(BF16)
            row = pl.multiple_of(g * 16, 16)
            for h in range(32):
                counts[h // 8, pl.ds(row, 16), (h % 8) * 128 : (h % 8 + 1) * 128] = r[h * 16 : (h + 1) * 16]
            return 0

        lax.fori_loop(0, 32, group, 0, unroll=8)

    def build_place(t):
        rep8 = one_hot(iota((W, 256), 0) == iota((W, 256), 1) % CAP + t * CAP)
        wide_in = dot(exact_bf16(in_block[...]), rep8)
        for g in range(GROUPS):
            jj = iota((N, 256), 0) - g * 32
            here = jj == iota((N, 256), 1) // CAP
            part = exact_bf16(jnp.where(here, wide_in, 0.0))
            inside = dot(jnp.ones((8, N), BF16), part)
            offset = (iota((8, 256), 1) // CAP * BLOCK).astype(F32)
            place[g] = jnp.where(inside < -0.5, -1.0, inside + offset).astype(I32)
            inside = dot_tn(part, jnp.ones((N, W), BF16))
            offset = (iota((256, W), 0) // CAP * BLOCK).astype(F32)
            placec[g] = jnp.where(inside < -0.5, -1.0, inside + offset).astype(I32)

    def build_sel(t):
        build_place(t)

        def group(g, _):
            s = one_hot(iota((1024, 256), 0) == place[g, :1, :])
            sel[t, g] = s
            gone[t, g] = dot(s, jnp.ones((256, W), BF16))
            return 0

        lax.fori_loop(0, GROUPS, group, 0, unroll=2)

    def build_flush_plan(t):
        def group(g, _):
            s = sel[t, g]
            mix[g] = dot(counts[g], s).astype(BF16).T
            st = one_hot(iota((256, 1024), 1) == placec[g, :, :1])
            base[g] = joined(dot(st, parts(waiting[pl.ds(pl.multiple_of(g * 1024, 1024), 1024), :])))
            return 0

        lax.fori_loop(0, GROUPS, group, 0, unroll=2)

    def pooled_base(masked_by):
        total = jnp.zeros((BAGS, 2 * W), F32)
        for g in range(GROUPS):
            c = cache[g * 1024 : (g + 1) * 1024, :]
            if masked_by is not None:
                c = jnp.where(gone[masked_by, g] > 0.5, 0.0, c)
            total = total + dot(counts[g], parts(c))
        return joined(total)

    def build_pick(t_prev):
        def group(g, _):
            pick[g] = dot(counts[g], sel[t_prev, g]).astype(BF16)
            return 0

        lax.fori_loop(0, GROUPS, group, 0, unroll=2)

    def update_waiting(t):
        def group(g, _):
            at = pl.ds(pl.multiple_of(g * 1024, 1024), 1024)
            w = waiting[at, :] + joined(dot_tn(counts[g], bag_grad[...]))
            waiting[at, :] = jnp.where(gone[t, g] > 0.5, 0.0, w)
            return 0

        lax.fori_loop(0, GROUPS, group, 0, unroll=2)

    def update_cache(t):
        def group(g, _):
            at = pl.ds(pl.multiple_of(g * 1024, 1024), 1024)
            new = joined(dot(sel[t, g], freshp[g]))
            cache[at, :] = jnp.where(gone[t, g] > 0.5, new, cache[at, :])
            return 0

        lax.fori_loop(0, GROUPS, group, 0, unroll=2)

    def send_quarter(q, src, dst, send_sem, recv_sem):
        def one(p):
            pltpu.make_async_remote_copy(
                src_ref=src.at[p], dst_ref=dst.at[me], send_sem=send_sem, recv_sem=recv_sem,
                device_id=p, device_id_type=LOGICAL,
            ).start()

        each_partner(q, one)

    def exchange_start(src, dst, send_sem, recv_sem):
        for q in far:
            send_quarter(q, src, dst, send_sem, recv_sem)
        dst[me] = src[me]

    def exchange_wait(src, dst, send_sem, recv_sem):
        all_of = pltpu.make_async_remote_copy(
            src_ref=src.at[pl.ds(0, N - 1)], dst_ref=dst.at[pl.ds(0, N - 1)], send_sem=send_sem,
            recv_sem=recv_sem, device_id=lax.rem(me + 1, N), device_id_type=LOGICAL,
        )
        all_of.wait_send()
        all_of.wait_recv()

    def plan_rows(t):
        x = jnp.broadcast_to(idx_recv[...], (N, CAP, W)).reshape(N * CAP, W)
        e = iota((N * CAP, W), 0)
        mine = iota((N * CAP, W), 1) == t * CAP + e % CAP
        col = jnp.sum(jnp.where(mine, x, 0).astype(F32), axis=1, keepdims=True)
        wide = jnp.broadcast_to(col, (N * CAP, W))
        ycol[t] = wide.astype(I32)
        for b in range(8):
            turned = wide[b * 128 : (b + 1) * 128, :].T
            yrow[t, :, b * 128 : (b + 1) * 128] = turned[:8, :].astype(I32)
        y = yrow[t, :1, :]

        def chunk(c, _):
            at = pl.ds(pl.multiple_of(c * 256, 256), 256)
            m = one_hot(ycol[t, at, :1] == y)
            same[at, :] = m
            share[at, :] = 1.0 / dot(m, jnp.ones((1024, W), BF16))
            return 0

        lax.fori_loop(0, 4, chunk, 0, unroll=2)

    def plan_values(t):
        yc = ycol[t]
        head = yc // 128
        hot = one_hot(iota((N * CAP, W), 1) == head)[:, :64]
        got = joined(dot(hot, parts(accum_out[...])))
        got = jnp.where(iota((N * CAP, W), 1) == yc - head * 128, got, 0.0)
        acc = jnp.sum(got, axis=1, keepdims=True)
        acc_old[...] = jnp.broadcast_to(jnp.where(yc[:, :1] >= ROWS, 1.0, acc), (N * CAP, W))

        def fetch(src, _):
            for k in range(CAP):
                i = jnp.clip(idx_sm[src, 0, t * CAP + k], 0, ROWS - 1)
                old[pl.ds(src * CAP + k, 1), :] = table[pl.ds(i, 1), :]
            return 0

        lax.fori_loop(0, N, fetch, 0, unroll=4)
        if t > 0:

            def correct(c, _):
                at = pl.ds(pl.multiple_of(c * 256, 256), 256)
                moved = jnp.zeros((256, 2 * W), F32)
                for s in range(t):
                    m = one_hot(ycol[t, at, :1] == yrow[s, :1, :])
                    moved = moved + dot(m, deltap[s])
                old[at, :] = old[at, :] - joined(moved)
                return 0

            lax.fori_loop(0, 4, correct, 0, unroll=2)

    def owner_update(t):
        gotp[...] = parts(recv_f[t].reshape(N * CAP, W))
        for q in far:
            base_src = lax.rem(quarter + q, 4) * 32
            at = pl.ds(pl.multiple_of(base_src * CAP, 256), 256)
            total = joined(dot(same[at, :], gotp[...]))
            extra = jnp.mean(total * total, axis=1, keepdims=True)
            step = total * (LEARN_RATE * lax.rsqrt(acc_old[at, :] + extra))
            send_b[t, pl.ds(base_src, 32)] = (old[at, :] - step).reshape(32, CAP, W)
            deltap[t, at, :] = parts(step * share[at, :])
            more[at, :] = extra * share[at, :]
            send_quarter(q, send_b.at[t], recv_b.at[t], bsend_sem.at[t], brecv_sem.at[t])
        recv_b[t, me] = send_b[t, me]

    def accum_update(t):
        y = yrow[t, :1, :]
        yc = ycol[t]
        tail = jnp.where(iota((N * CAP, W), 1) == yc - yc // 128 * 128, more[...], 0.0)
        hot = one_hot(iota((64, N * CAP), 0) == y // 128)
        accum_out[...] = accum_out[...] + joined(dot(hot, parts(tail)))

    accum_out[...] = accum_ref[...]
    stores = []
    build_counts(0)
    pl.semaphore_wait(barrier, N - 1)
    exchange_start(idx_send, idx_recv, isend_sem.at[0], irecv_sem.at[0])
    build_sel(0)
    loads[0].wait()
    pooled = pooled_base(None)
    loads[2].wait()
    build_flush_plan(0)
    loads[1].wait()
    inv_copy.wait()
    for t in range(STEPS):
        if t > 0:
            moved = dot(pick[0], freshp[0])
            for g in range(1, GROUPS):
                moved = moved + dot(pick[g], freshp[g])
            pooled = base_pooled + joined(moved)
        grad = (pooled * (1.0 / BAG) - targets[t]) * (1.0 / BAG)
        bag_grad[...] = parts(grad)
        for g in range(GROUPS):
            out = base[g] + joined(dot(mix[g], bag_grad[...]))
            flush[g * 32 : (g + 1) * 32] = out.reshape(32, CAP, W)

        for n, q in enumerate((*far, None)):
            if q is not None:
                first = lax.rem(quarter + q, 4) * 32

                def to_owner(o, _):
                    send_f[t, first + o] = flush[jnp.clip(inv_sm[0, first + o], 0, N - 1)]
                    return 0

                lax.fori_loop(0, 32, to_owner, 0, unroll=8)
            if n > 0:
                send_quarter(far[n - 1], send_f.at[t], recv_f.at[t], fsend_sem.at[t], frecv_sem.at[t])
        recv_f[t, me] = send_f[t, me]
        update_waiting(t)
        if t == STEPS - 1:
            pending_store = pltpu.make_async_copy(waiting, pending_out, out_sem.at[0])
            pending_store.start()
            stores.append(pending_store)
        if t == 0:
            exchange_wait(idx_send, idx_recv, isend_sem.at[0], irecv_sem.at[0])
            idx_copy = pltpu.make_async_copy(idx_recv, idx_sm, sm_sem.at[1])
            idx_copy.start()
            plan_rows(0)
            loads[3].wait()
            loads[4].wait()
            idx_copy.wait()
        plan_values(t)
        if t > 0:
            update_cache(t - 1)
        if t < STEPS - 1:
            build_counts(t + 1)
        exchange_wait(send_f.at[t], recv_f.at[t], fsend_sem.at[t], frecv_sem.at[t])
        owner_update(t)
        if t < STEPS - 1:
            build_sel(t + 1)
            build_pick(t)
            base_pooled = pooled_base(t)
            build_flush_plan(t + 1)
            plan_rows(t + 1)
        accum_update(t)
        answers = pltpu.make_async_copy(send_b.at[t], answers_out.at[t], out_sem.at[2 + t])
        answers.start()
        stores.append(answers)
        if t == 0:
            idx_store = pltpu.make_async_copy(idx_recv, idx_out, out_sem.at[1])
            idx_store.start()
            stores.append(idx_store)
        exchange_wait(send_b.at[t], recv_b.at[t], bsend_sem.at[t], brecv_sem.at[t])

        def from_owner(j, _):
            fresh[j] = recv_b[t, jnp.clip(lax.div(held_sm[j * BLOCK], ROWS), 0, N - 1)]
            return 0

        lax.fori_loop(0, N, from_owner, 0, unroll=8)
        for g in range(GROUPS):
            freshp[g] = parts(fresh[g * 32 : (g + 1) * 32].reshape(256, W))
    update_cache(STEPS - 1)
    cache_store = pltpu.make_async_copy(cache, cache_out, out_sem.at[5])
    cache_store.start()
    stores.append(cache_store)
    for store in stores:
        store.wait()


def finish(
    idx_hbm, accum_in, table_hbm, answers_hbm, cache_hbm, pending_hbm,
    accum_out, table_out, cache_out, pending_out,
    table, answers, cache, pending, idx_sm, in_sem, out_sem,
):
    loads = [
        pltpu.make_async_copy(answers_hbm, answers, in_sem.at[0]),
        pltpu.make_async_copy(table_hbm, table.at[pl.ds(0, ROWS)], in_sem.at[1]),
        pltpu.make_async_copy(cache_hbm, cache, in_sem.at[2]),
        pltpu.make_async_copy(pending_hbm, pending, in_sem.at[3]),
        pltpu.make_async_copy(idx_hbm, idx_sm, in_sem.at[4]),
    ]
    loads[4].start()
    for load in loads[:4]:
        load.start()
    accum_out[...] = accum_in[...]
    loads[0].wait()
    loads[1].wait()
    loads[4].wait()
    for t in range(STEPS):

        def rows_of(src, _):
            for k in range(CAP):
                table[pl.ds(idx_sm[src, 0, t * CAP + k], 1), :] = answers[t, src, k : k + 1, :]
            return 0

        lax.fori_loop(0, N, rows_of, 0, unroll=4)
        if t == 0:
            loads[2].wait()
            cache_store = pltpu.make_async_copy(cache, cache_out, out_sem.at[0])
            cache_store.start()
            loads[3].wait()
            pending_store = pltpu.make_async_copy(pending, pending_out, out_sem.at[1])
            pending_store.start()
    table_store = pltpu.make_async_copy(table.at[pl.ds(0, ROWS)], table_out, out_sem.at[2])
    table_store.start()
    cache_store.wait()
    pending_store.wait()
    table_store.wait()


def body(table, accum, cache_values, cache_rows, pending, batch_slots, targets, dirty):
    keys = batch_slots.reshape(STEPS, 32, 256)
    rows = cache_rows.reshape(32, 128)
    vmem = pl.BlockSpec(memory_space=pltpu.VMEM)
    hbm = pl.BlockSpec(memory_space=pl.ANY)
    dma = pltpu.SemaphoreType.DMA
    tiles = (N, CAP, W)
    answers, idx, new_accum, new_cache, new_pending = pl.pallas_call(
        kernel,
        out_shape=(
            jax.ShapeDtypeStruct((STEPS, *tiles), F32),
            jax.ShapeDtypeStruct((N, 1, W), I32),
            jax.ShapeDtypeStruct((64, W), F32),
            jax.ShapeDtypeStruct((SLOTS, W), F32),
            jax.ShapeDtypeStruct((SLOTS, W), F32),
        ),
        in_specs=[hbm, vmem, vmem, vmem, vmem, hbm, hbm, hbm, hbm],
        out_specs=(hbm, hbm, vmem, hbm, hbm),
        scratch_shapes=[
            pltpu.VMEM((ROWS, W), F32),
            pltpu.VMEM((SLOTS, W), F32),
            pltpu.VMEM((SLOTS, W), F32),
            pltpu.VMEM((STEPS, BAGS, W), F32),
            pltpu.VMEM((GROUPS, BAGS, 1024), BF16),
            pltpu.VMEM((STEPS, GROUPS, 1024, 256), BF16),
            pltpu.VMEM((GROUPS, 256, BAGS), BF16),
            pltpu.VMEM((GROUPS, BAGS, 256), BF16),
            pltpu.VMEM((GROUPS, 256, W), F32),
            pltpu.VMEM(tiles, F32),
            pltpu.VMEM(tiles, F32),
            pltpu.VMEM((GROUPS, 256, 2 * W), BF16),
            pltpu.VMEM((BAGS, 2 * W), BF16),
            pltpu.VMEM((STEPS, *tiles), F32),
            pltpu.VMEM((STEPS, *tiles), F32),
            pltpu.VMEM((STEPS, *tiles), F32),
            pltpu.VMEM((STEPS, *tiles), F32),
            pltpu.VMEM((N, 1, W), I32),
            pltpu.VMEM((N, 1, W), I32),
            pltpu.SMEM((N, 1, W), I32),
            pltpu.VMEM((8, N), I32),
            pltpu.SMEM((8, N), I32),
            pltpu.SMEM((SLOTS,), I32),
            pltpu.VMEM((N, W), F32),
            pltpu.VMEM((GROUPS, 8, 256), I32),
            pltpu.VMEM((GROUPS, 256, W), I32),
            pltpu.VMEM((STEPS, N * CAP, W), I32),
            pltpu.VMEM((STEPS, 8, N * CAP), I32),
            pltpu.VMEM((N * CAP, N * CAP), BF16),
            pltpu.VMEM((N * CAP, W), F32),
            pltpu.VMEM((N * CAP, W), F32),
            pltpu.VMEM((N * CAP, W), F32),
            pltpu.VMEM((STEPS, GROUPS, 1024, W), F32),
            pltpu.VMEM((N * CAP, 2 * W), BF16),
            pltpu.VMEM((STEPS, N * CAP, 2 * W), BF16),
            pltpu.VMEM((N * CAP, W), F32),
            dma((5,)),
            dma((2,)),
            dma((6,)),
            dma((1,)),
            dma((1,)),
            dma((STEPS,)),
            dma((STEPS,)),
            dma((STEPS,)),
            dma((STEPS,)),
        ],
        compiler_params=pltpu.CompilerParams(
            collective_id=0, has_side_effects=True, vmem_limit_bytes=56 * 1024 * 1024
        ),
    )(
        cache_rows, keys, dirty, rows, accum.reshape(64, W), table, cache_values, pending, targets
    )
    new_accum, new_table, new_cache, new_pending = pl.pallas_call(
        finish,
        out_shape=(
            jax.ShapeDtypeStruct((64, W), F32),
            jax.ShapeDtypeStruct((ROWS, W), F32),
            jax.ShapeDtypeStruct((SLOTS, W), F32),
            jax.ShapeDtypeStruct((SLOTS, W), F32),
        ),
        in_specs=[hbm, vmem, hbm, hbm, hbm, hbm],
        out_specs=(vmem, hbm, hbm, hbm),
        scratch_shapes=[
            pltpu.VMEM((ROWS + 8, W), F32),
            pltpu.VMEM((STEPS, *tiles), F32),
            pltpu.VMEM((SLOTS, W), F32),
            pltpu.VMEM((SLOTS, W), F32),
            pltpu.SMEM((N, 1, W), I32),
            dma((5,)),
            dma((3,)),
        ],
    )(idx, new_accum, table, answers, new_cache, new_pending)
    return new_table, new_accum.reshape(-1), new_cache, new_pending


def solution(mesh):
    in_specs = (
        P(("gx", "gy"), None),
        P(("gx", "gy")),
        P(("gx", "gy"), None),
        P(("gx", "gy")),
        P(("gx", "gy"), None),
        P(None, ("gx", "gy"), None),
        P(None, ("gx", "gy"), None),
        P(None, ("gx", "gy")),
    )
    out_specs = (
        P(("gx", "gy"), None),
        P(("gx", "gy")),
        P(("gx", "gy"), None),
        P(("gx", "gy"), None),
    )
    return jax.shard_map(body, mesh=mesh, in_specs=in_specs, out_specs=out_specs, check_vma=False)
```
